256 devices in a mesh: row: 8 (over z_hi, core), sa: 32 (over z_lo, x, y).
Axes of the slice: x: 4, y: 4, z: 8 (z_hi: 4, z_lo: 2; z = z_hi * 2 + z_lo), core: 2. Of those that a mesh axis runs over, the one named last changes fastest.
Arguments:
- rep_w1: float32 [16, 8, 128, 4096], P('row', None, None, 'sa'), may hold values from -6 to 6
- rep_w3: float32 [16, 8, 128, 4096], P('row', None, None, 'sa'), may hold values from -6 to 6
- rep_w2: float32 [16, 8, 128, 4096], P('row', None, None, 'sa'), may hold values from -6 to 6
- rep_gate: float32 [16, 8, 4096], P('row', None, 'sa'), may hold values from -6 to 6
Outputs:
- serve_w1: bfloat16 [8, 128, 4096], P('row', 'sa')
- serve_w3: bfloat16 [8, 128, 4096], P('row', 'sa')
- serve_w2: bfloat16 [8, 128, 4096], P('row', 'sa')
- serve_gate: bfloat16 [8, 4096], replicated
- soup_norms: float32 [8, 4], P('row')
- replica_norms: float32 [16, 8, 4], P('row')
The draws below stay inside these ranges and needn't reach their ends.
All inputs are finite; a program needn't handle non-finite values.
Results may differ from the reference program's by a relative error of at most 0.001.
Values may be sent and summed in bfloat16 or wider, within the bound.
A program may use at most 64 MiB of HBM per device.

```python
import jax
import jax.numpy as jnp
from jax import lax

D = 4096
EXPERTS = 8
REPLICAS = 16
HID = 128


def raised(drawn, key, source, target, blocks, factor):
    def block_of(axis_at):
        return (jnp.arange(drawn.shape[axis_at]) // (drawn.shape[axis_at] // blocks)).reshape((-1,) + (1,) * (drawn.ndim - 1 - axis_at))

    first = jax.random.permutation(key, blocks)[block_of(target)]
    other_side = (block_of(target) + blocks // 2) % blocks
    return jnp.where((block_of(source) == first) | (block_of(source) == other_side), factor * drawn, drawn)


def block_scale(stream_key, shape, cuts, low, largest):
    def one(axis_at, blocks):
        draws = jax.random.uniform(jax.random.fold_in(jax.random.fold_in(stream_key, 6), axis_at), (blocks,), jnp.float32, low / len(cuts), largest / len(cuts))
        return jnp.repeat(jnp.exp(draws), shape[axis_at] // blocks).reshape((-1,) + (1,) * (len(shape) - axis_at - 1))

    factor_of = one(*cuts[0])
    for cut in cuts[1:]:
        factor_of = factor_of * one(*cut)
    return factor_of


def heavy_noise(own_key, dims, width, limit, shards, heavy, dtype=jnp.bfloat16):
    drawn = width * jax.random.normal(own_key, dims, jnp.float32)
    if shards:
        drawn = drawn * block_scale(own_key, dims, shards, -0.22, 0.18)
    return jnp.clip(raised(drawn, jax.random.fold_in(own_key, 3), *heavy), -limit, limit).astype(dtype)


def setup_inputs(seed: int = 0) -> dict:
    streams_of = jax.random.split(jax.random.key(seed), 5)
    rep_w1 = heavy_noise(streams_of[0], (REPLICAS, EXPERTS, HID, D), 1.0, 6.0, ((0, 8), (3, 32)), (3, 0, 16, 2.0), jnp.float32)
    rep_w3 = heavy_noise(streams_of[1], (REPLICAS, EXPERTS, HID, D), 1.0, 6.0, ((0, 8), (3, 32)), (3, 0, 16, 2.0), jnp.float32)
    rep_w2 = heavy_noise(streams_of[2], (REPLICAS, EXPERTS, HID, D), 1.0, 6.0, ((0, 8), (3, 32)), (3, 0, 16, 2.0), jnp.float32)
    rep_gate = heavy_noise(streams_of[3], (REPLICAS, EXPERTS, D), 1.0, 6.0, ((0, 8), (2, 32)), (2, 0, 16, 2.0), jnp.float32)
    return {"rep_w1": rep_w1, "rep_w3": rep_w3, "rep_w2": rep_w2, "rep_gate": rep_gate}


def square_sums(values, dims_summed):
    return lax.optimization_barrier(jnp.sum(values * values, axis=dims_summed))

def reference(rep_w1, rep_w3, rep_w2, rep_gate):
    weights = (rep_w1, rep_w3, rep_w2)
    served_list = []
    for weight in weights:
        soup = lax.optimization_barrier(jnp.sum(weight, axis=0)) / REPLICAS
        served_list.append(soup.astype(jnp.bfloat16))
    gate_soup = lax.optimization_barrier(jnp.sum(rep_gate, axis=0)) / REPLICAS
    serve_gate = gate_soup.astype(jnp.bfloat16)
    expert_entries = HID * D
    soup_columns = [jnp.sqrt(square_sums(served.astype(jnp.float32), (1, 2)) / expert_entries) for served in served_list]
    soup_columns.append(jnp.sqrt(square_sums(serve_gate.astype(jnp.float32), 1) / D))
    soup_norms = jnp.stack(soup_columns, axis=1)
    replica_columns = [jnp.sqrt(square_sums(weight, (2, 3)) / expert_entries) for weight in weights]
    replica_columns.append(jnp.sqrt(square_sums(rep_gate, 2) / D))
    replica_norms = jnp.stack(replica_columns, axis=2)
    return (served_list[0], served_list[1], served_list[2], serve_gate, soup_norms, replica_norms)
```

```python
import functools

import jax
import jax.numpy as jnp
from jax import lax
from jax.experimental import pallas as pl
from jax.experimental.pallas import tpu as pltpu
from jax.sharding import PartitionSpec as P

MESH = pl.DeviceIdType.MESH
F32, BF16 = jnp.float32, jnp.bfloat16

SPAN = 2.0**7.875


def row_max(block8):
    return jnp.maximum(jnp.max(block8, axis=0, keepdims=True), 1e-30)


def round_up(scale):
    return (scale * 1.015625).astype(BF16)


def encoded(values, factor):
    u = values * factor
    u2 = u * u
    u4 = u2 * u2
    u8 = u4 * u4
    u16 = u8 * u8
    return jnp.where(u < 0, -u16, u16).astype(BF16)


def decoded(wire, factor):
    y = wire.astype(F32)
    root = lax.rsqrt(lax.rsqrt(lax.rsqrt(lax.rsqrt(jnp.abs(y)))))
    return jnp.where(y < 0, -root, root) * factor


def kernel(
    w1, w3, w2, gate,
    out_w1, out_w3, out_w2, out_gate, out_soup, out_rep,
    load, gload, sown, dsend, drecv, squares, rowsums,
    zsend, zrecv, gall, gdrecv, gshard, served, msgs, recv,
    load_sem, gload_sem, ds_sem, dr_sem, zs_sem, zr_sem, gd_sem, gz_sem, ga_sem, ms_sem, mr_sem,
):
    weights = (w1, w3, w2)
    row, sa = lax.axis_index("row"), lax.axis_index("sa")
    zh, core = row // 2, row % 2
    partner = row + 1 - 2 * core
    up, down = (row + 2) % 8, (row + 6) % 8

    chips = [(zh + d) % 4 for d in (2, 1, 3, 0)]

    def load_copy(k, t):
        return pltpu.make_async_copy(
            weights[t].at[:, pl.ds(2 * chips[k], 2)], load.at[k, t], load_sem.at[k, t]
        )

    gate_load = pltpu.make_async_copy(gate, gload, gload_sem)
    for t in range(3):
        load_copy(0, t).start()
    gate_load.start()

    barrier = pltpu.get_barrier_semaphore()
    for peer in (partner, up, down):
        pl.semaphore_signal(barrier, inc=1, device_id=(peer, sa), device_id_type=MESH)

    def greet(i, _):
        pl.semaphore_signal(barrier, inc=1, device_id=(row, (sa + i) % 32), device_id_type=MESH)
        return 0

    lax.fori_loop(1, 32, greet, 0)
    for k in range(1, 4):
        for t in range(3):
            load_copy(k, t).start()

    def chunk_sums(k, parity, dest):
        expert = 2 * chips[k] + parity
        top = jnp.zeros((8, 128), F32)
        for t in range(3):
            a, b = load[k, t, 0, parity], load[k, t, 1, parity]
            total = a + b
            dest[t * 128 : (t + 1) * 128, :] = total
            for r, v in ((0, a), (1, b)):
                index = pl.multiple_of((t * 16 + r * 8 + expert) * 8, 8)
                squares[pl.ds(index, 8), :] = jnp.sum((v * v).reshape(16, 8, 128), axis=0)
            if k < 3:
                top = jnp.maximum(top, jnp.max(jnp.abs(total).reshape(16, 8, 128), axis=0))
        if k < 3:
            dest[384:392, :] = top

    def d2d(k):
        return pltpu.make_async_remote_copy(
            src_ref=dsend.at[k], dst_ref=drecv.at[k], send_sem=ds_sem.at[k], recv_sem=dr_sem.at[k],
            device_id=(partner, sa), device_id_type=MESH,
        )

    def z_copy(way, stage, piece):
        rows = pl.ds(0, 80) if piece == 0 else pl.ds(16 + 64 * piece, 64)
        return pltpu.make_async_remote_copy(
            src_ref=zsend.at[way, stage, rows], dst_ref=zrecv.at[way, stage, rows],
            send_sem=zs_sem.at[way, stage, piece], recv_sem=zr_sem.at[way, stage, piece],
            device_id=((up, down)[way], sa), device_id_type=MESH,
        )

    def chip_rows(k, t, half):
        rows = slice(t * 128 + half * 64, t * 128 + half * 64 + 64)
        return sown[k, rows, :] + drecv[k, rows, :]

    def chip_top(k):
        return row_max(sown[k, 384:392, :] + drecv[k, 384:392, :])

    def put_scale(way, stage, scale):
        zsend[way, stage, 0:16, :] = jnp.broadcast_to(scale, (16, 128))
        return SPAN / scale.astype(F32)

    def z_piece(way, stage, t, values, factor):
        zsend[way, stage, 16 + 64 * t : 80 + 64 * t, :] = encoded(values, factor)
        z_copy(way, stage, t).start()

    def z_scale(way, stage):
        return zrecv[way, stage, 0:16, :].astype(F32)[0:1]

    def z_values(way, stage, t):
        return decoded(
            zrecv[way, stage, 16 + 64 * t : 80 + 64 * t, :], z_scale(way, stage) * (1 / SPAN)
        )

    def prepare(k):
        for t in range(3):
            load_copy(k, t).wait()
        chunk_sums(k, 1 - core, dsend.at[k])
        if k == 0:
            pl.semaphore_wait(barrier, 34)
        d2d(k).start()
        chunk_sums(k, core, sown.at[k])

    def gate_d2d():
        return pltpu.make_async_remote_copy(
            src_ref=gall.at[4], dst_ref=gdrecv, send_sem=gd_sem.at[0], recv_sem=gd_sem.at[1],
            device_id=(partner, sa), device_id_type=MESH,
        )

    def gate_copy(which):
        slot = (zh, zh, (zh + 3) % 4)[which]
        return pltpu.make_async_remote_copy(
            src_ref=gall.at[slot], dst_ref=gall.at[slot],
            send_sem=gz_sem.at[0, which], recv_sem=gz_sem.at[1, which],
            device_id=((up, down, up)[which], sa), device_id_type=MESH,
        )

    prepare(0)

    gate_load.wait()
    gall[4] = gload[0] + gload[1]
    gate_d2d().start()
    for r in range(2):
        rowsums[48 + 8 * r : 56 + 8 * r, :] = gload[r] * gload[r]

    prepare(1)

    d2d(0).wait_recv()
    scale = round_up(chip_top(0))
    factors = [put_scale(way, 0, scale) for way in range(2)]
    for t in range(3):
        for way in range(2):
            z_piece(way, 0, t, chip_rows(0, t, way), factors[way])

    gate_d2d().wait_recv()
    gall[zh] = gall[4] + gdrecv[...]
    gate_copy(0).start()
    gate_copy(1).start()

    prepare(2)

    tops = []
    for way in range(2):
        k = 1 + way
        d2d(k).wait_recv()
        tops.append(chip_top(k))
        factor = put_scale(way, 1, round_up(tops[way]))
        for t in range(3):
            z_piece(way, 1, t, chip_rows(k, t, 1 - way), factor)

    prepare(3)

    factors = []
    for t in range(3):
        for way in range(2):
            z_copy(way, 0, t).wait_recv()
            if t == 0:
                scale = round_up(tops[way] + z_scale(way, 0))
                factors.append(put_scale(way, 2, scale))
            values = chip_rows(1 + way, t, way) + z_values(way, 0, t)
            z_piece(way, 2, t, values, factors[way])

    gate_copy(0).wait_recv()
    gate_copy(2).start()
    gate_copy(1).wait_recv()
    gate_copy(2).wait_recv()
    gate_total = ((gall[0] + gall[1]) + gall[2]) + gall[3]
    gshard[...] = (gate_total * (1 / 16)).astype(BF16)

    def gate_send(i):
        return pltpu.make_async_remote_copy(
            src_ref=gshard, dst_ref=out_gate.at[:, pl.ds(pl.multiple_of(sa * 128, 128), 128)],
            send_sem=ga_sem.at[0], recv_sem=ga_sem.at[1],
            device_id=(row, (sa + i) % 32), device_id_type=MESH,
        )

    def gate_start(i, _):
        gate_send(i).start()
        return 0

    lax.fori_loop(1, 32, gate_start, 0)
    out_gate[:, pl.ds(pl.multiple_of(sa * 128, 128), 128)] = gshard[...]

    for t in range(3):
        part = squares[pl.ds(t * 128, 16, stride=8), :]
        for j in range(1, 8):
            part = part + squares[pl.ds(t * 128 + j, 16, stride=8), :]
        rowsums[16 * t : 16 * t + 16, :] = part
    rowsums[64:128, :] = jnp.zeros((64, 128), F32)
    norm_row = jnp.sum(rowsums[...].T, axis=0, keepdims=True)
    lane = lax.broadcasted_iota(jnp.int32, (1, 128), 1)

    d2d(3).wait_recv()
    for t in range(3):
        for half in range(2):
            total = chip_rows(3, t, half)
            z_copy(1 - half, 1, t).wait_recv()
            total = total + z_values(1 - half, 1, t)
            z_copy(half, 2, t).wait_recv()
            total = total + z_values(half, 2, t)
            served[t, 64 * half : 64 * half + 64, :] = (total * (1 / 16)).astype(BF16).astype(F32)
        final = served[t]
        square = jnp.sum(final * final, axis=(0, 1), keepdims=True)
        norm_row = jnp.where(lane == 64 + t, square, norm_row)

    high = norm_row.astype(BF16).astype(F32)
    rest = norm_row - high
    middle = rest.astype(BF16).astype(F32)
    tail = jnp.concatenate([high, middle, rest - middle, jnp.zeros((1, 128), F32)], axis=0)
    for p in range(32):
        parts = [served[t, 4 * p : 4 * p + 4, :] for t in range(3)]
        msgs[p] = jnp.concatenate(parts + [tail], axis=0).astype(BF16)

    def msg_send(i):
        return pltpu.make_async_remote_copy(
            src_ref=msgs.at[(sa + i) % 32], dst_ref=recv.at[sa],
            send_sem=ms_sem, recv_sem=mr_sem,
            device_id=(row, (sa + i) % 32), device_id_type=MESH,
        )

    def msg_start(i, _):
        msg_send(i).start()
        return 0

    lax.fori_loop(1, 32, msg_start, 0)
    recv[sa] = msgs[sa]

    for k in range(4):
        d2d(k).wait_send()
    for way in range(2):
        for stage in range(3):
            for t in range(3):
                z_copy(way, stage, t).wait_send()
    gate_d2d().wait_send()
    for which in range(3):
        gate_copy(which).wait_send()
    others = out_gate.at[:, pl.ds(0, 31 * 128)]
    pltpu.make_async_copy(others, others, ga_sem.at[0]).wait()
    pltpu.make_async_copy(others, others, ga_sem.at[1]).wait()

    gates = out_gate[...].astype(F32)
    mine = lax.broadcasted_iota(jnp.int32, gates.shape, 0) == row
    gate_square = jnp.sum(jnp.where(mine, gates * gates, 0.0), axis=(0, 1), keepdims=True)

    batch = recv.at[pl.ds(0, 31)]
    pltpu.make_async_copy(batch, batch, ms_sem).wait()
    pltpu.make_async_copy(batch, batch, mr_sem).wait()

    totals = jnp.zeros((4, 128), F32)
    for s in range(32):
        message = recv[s].astype(F32)
        for t, out in enumerate((out_w1, out_w3, out_w2)):
            out[0, :, 128 * s : 128 * s + 128] = message[4 * t : 4 * t + 4].astype(BF16)
        totals = totals + message[12:16]
    total_row = (totals[0:1] + totals[1:2]) + totals[2:3]

    wide = jnp.broadcast_to(total_row, (16, 128))
    lanes = lax.broadcasted_iota(jnp.int32, (16, 128), 1)
    rows = lax.broadcasted_iota(jnp.int32, (16, 128), 0)
    spread = jnp.zeros((16, 128), F32)
    for t in range(4):
        column = jnp.sum(jnp.where(lanes == rows + 16 * t, wide, 0.0), axis=1, keepdims=True)
        spread = jnp.where(lanes == t, column * (1 / (4096 if t == 3 else 524288)), spread)
    norms = jnp.sqrt(spread)
    for r in range(2):
        out_rep[r] = norms[8 * r : 8 * r + 8, 0:4]

    soup = jnp.where(lane == 3, gate_square * (1 / 4096), 0.0)
    for t in range(3):
        entry = jnp.sum(jnp.where(lane == 64 + t, total_row, 0.0), axis=1, keepdims=True)
        soup = jnp.where(lane == t, entry * (1 / 524288), soup)
    out_soup[...] = jnp.sqrt(soup)[:, 0:4]


def body(w1, w3, w2, gate):
    vmem = pl.BlockSpec(memory_space=pltpu.VMEM)
    hbm = pl.BlockSpec(memory_space=pl.ANY)
    dma = pltpu.SemaphoreType.DMA
    return pl.pallas_call(
        kernel,
        name="soup",
        out_shape=(
            jax.ShapeDtypeStruct((1, 4, 4096), BF16),
            jax.ShapeDtypeStruct((1, 4, 4096), BF16),
            jax.ShapeDtypeStruct((1, 4, 4096), BF16),
            jax.ShapeDtypeStruct((8, 4096), BF16),
            jax.ShapeDtypeStruct((1, 4), F32),
            jax.ShapeDtypeStruct((2, 8, 4), F32),
        ),
        in_specs=[hbm] * 4,
        out_specs=(vmem,) * 6,
        scratch_shapes=[
            pltpu.VMEM((4, 3, 2, 2, 128, 128), F32),
            pltpu.VMEM((2, 8, 128), F32),
            pltpu.VMEM((4, 392, 128), F32),
            pltpu.VMEM((4, 392, 128), F32),
            pltpu.VMEM((4, 392, 128), F32),
            pltpu.VMEM((384, 128), F32),
            pltpu.VMEM((128, 128), F32),
            pltpu.VMEM((2, 3, 208, 128), BF16),
            pltpu.VMEM((2, 3, 208, 128), BF16),
            pltpu.VMEM((5, 8, 128), F32),
            pltpu.VMEM((8, 128), F32),
            pltpu.VMEM((8, 128), BF16),
            pltpu.VMEM((3, 128, 128), F32),
            pltpu.VMEM((32, 16, 128), BF16),
            pltpu.VMEM((32, 16, 128), BF16),
            dma((4, 3)),
            dma,
            dma((4,)),
            dma((4,)),
            dma((2, 3, 3)),
            dma((2, 3, 3)),
            dma((2,)),
            dma((2, 3)),
            dma((2,)),
            dma,
            dma,
        ],
        compiler_params=pltpu.CompilerParams(collective_id=0, has_side_effects=True),
    )(w1, w3, w2, gate)


def solution(mesh):
    in_specs = (
        P("row", None, None, "sa"),
        P("row", None, None, "sa"),
        P("row", None, None, "sa"),
        P("row", None, "sa"),
    )
    out_specs = (
        P("row", "sa", None),
        P("row", "sa", None),
        P("row", "sa", None),
        P(),
        P("row", None),
        P("row", None, None),
    )
    return jax.shard_map(body, mesh=mesh, in_specs=in_specs, out_specs=out_specs, check_vma=False)
```

```python
import functools

import jax
import jax.numpy as jnp
from jax import lax
from jax.experimental import pallas as pl
from jax.experimental.pallas import tpu as pltpu
from jax.sharding import PartitionSpec as P

MESH = pl.DeviceIdType.MESH
F32, BF16 = jnp.float32, jnp.bfloat16

SPAN = 2.0**7.875


def row_max(block8):
    return jnp.maximum(jnp.max(block8, axis=0, keepdims=True), 1e-30)


def round_up(scale):
    return (scale * 1.015625).astype(BF16)


def encoded(values, factor):
    u = values * factor
    u2 = u * u
    u4 = u2 * u2
    u8 = u4 * u4
    u16 = u8 * u8
    return jnp.where(u < 0, -u16, u16).astype(BF16)


def decoded(wire, factor):
    y = wire.astype(F32)
    root = lax.rsqrt(lax.rsqrt(lax.rsqrt(lax.rsqrt(jnp.abs(y)))))
    return jnp.where(y < 0, -root, root) * factor


def kernel(
    w1, w3, w2, gate,
    recv, out_gate,
    load, gload, sown, dsend, drecv, squares, rowsums,
    zsend, zrecv, gall, gdrecv, gshard, served, msgs,
    load_sem, gload_sem, ds_sem, dr_sem, zs_sem, zr_sem, gd_sem, gz_sem, ga_sem, ms_sem, mr_sem, known,
):
    weights = (w1, w3, w2)
    row, sa = lax.axis_index("row"), lax.axis_index("sa")
    zh, core = row // 2, row % 2
    partner = row + 1 - 2 * core
    up, down = (row + 2) % 8, (row + 6) % 8

    chips = [(zh + d) % 4 for d in (2, 1, 3, 0)]

    def load_copy(k, t):
        return pltpu.make_async_copy(
            weights[t].at[:, pl.ds(2 * chips[k], 2)], load.at[k, t], load_sem.at[k, t]
        )

    gate_load = pltpu.make_async_copy(gate, gload, gload_sem)
    gate_load.start()
    for t in range(3):
        load_copy(0, t).start()

    zl, x, y = sa // 16, (sa // 4) % 4, sa % 4
    x_line = [(row, zl * 16 + ((x + i) % 4) * 4 + y) for i in (1, 2, 3)]
    y_line = [(row, zl * 16 + x * 4 + (y + i) % 4) for i in (1, 2, 3)]
    z_pair = (row, sa + 16 - 32 * zl)
    barrier = pltpu.get_barrier_semaphore()
    for device in [(up, sa), (down, sa), (partner, sa), *x_line, *y_line, z_pair]:
        pl.semaphore_signal(barrier, inc=1, device_id=device, device_id_type=MESH)
    for k in range(1, 4):
        for t in range(3):
            load_copy(k, t).start()

    def chunk_sums(k, parity, dest):
        expert = 2 * chips[k] + parity
        top = jnp.zeros((8, 128), F32)
        for t in range(3):
            a, b = load[k, t, 0, parity], load[k, t, 1, parity]
            total = a + b
            dest[t * 128 : (t + 1) * 128, :] = total
            for r, v in ((0, a), (1, b)):
                index = pl.multiple_of((t * 16 + r * 8 + expert) * 8, 8)
                squares[pl.ds(index, 8), :] = jnp.sum((v * v).reshape(16, 8, 128), axis=0)
            if k < 3:
                top = jnp.maximum(top, jnp.max(jnp.abs(total).reshape(16, 8, 128), axis=0))
        if k < 3:
            dest[384:392, :] = top

    def d2d(k):
        return pltpu.make_async_remote_copy(
            src_ref=dsend.at[k], dst_ref=drecv.at[k], send_sem=ds_sem.at[k], recv_sem=dr_sem.at[k],
            device_id=(partner, sa), device_id_type=MESH,
        )

    def z_copy(way, stage, piece):
        rows = pl.ds(0, 80) if piece == 0 else pl.ds(16 + 64 * piece, 64)
        return pltpu.make_async_remote_copy(
            src_ref=zsend.at[way, stage, rows], dst_ref=zrecv.at[way, stage, rows],
            send_sem=zs_sem.at[way, stage, piece], recv_sem=zr_sem.at[way, stage, piece],
            device_id=((up, down)[way], sa), device_id_type=MESH,
        )

    def chip_rows(k, t, half):
        rows = slice(t * 128 + half * 64, t * 128 + half * 64 + 64)
        return sown[k, rows, :] + drecv[k, rows, :]

    def chip_top(k):
        return row_max(sown[k, 384:392, :] + drecv[k, 384:392, :])

    def put_scale(way, stage, scale):
        zsend[way, stage, 0:16, :] = jnp.broadcast_to(scale, (16, 128))
        return SPAN / scale.astype(F32)

    def z_piece(way, stage, t, values, factor):
        zsend[way, stage, 16 + 64 * t : 80 + 64 * t, :] = encoded(values, factor)
        z_copy(way, stage, t).start()

    def z_scale(way, stage):
        return zrecv[way, stage, 0:16, :].astype(F32)[0:1]

    def z_values(way, stage, t):
        return decoded(
            zrecv[way, stage, 16 + 64 * t : 80 + 64 * t, :], z_scale(way, stage) * (1 / SPAN)
        )

    def prepare(k):
        for t in range(3):
            load_copy(k, t).wait()
        chunk_sums(k, 1 - core, dsend.at[k])
        if k == 0:
            pl.semaphore_wait(barrier, 10)
            gate_d2d().start()
        d2d(k).start()
        if k == 0:
            for device in x_line:
                pl.semaphore_signal(known.at[0], inc=1, device_id=device, device_id_type=MESH)
        chunk_sums(k, core, sown.at[k])

    def gate_d2d():
        return pltpu.make_async_remote_copy(
            src_ref=gall.at[4], dst_ref=gdrecv, send_sem=gd_sem.at[0], recv_sem=gd_sem.at[1],
            device_id=(partner, sa), device_id_type=MESH,
        )

    def gate_copy(which):
        slot = (zh, zh, (zh + 3) % 4)[which]
        return pltpu.make_async_remote_copy(
            src_ref=gall.at[slot], dst_ref=gall.at[slot],
            send_sem=gz_sem.at[0, which], recv_sem=gz_sem.at[1, which],
            device_id=((up, down, up)[which], sa), device_id_type=MESH,
        )

    gate_load.wait()
    gall[4] = gload[0] + gload[1]
    for r in range(2):
        rowsums[48 + 8 * r : 56 + 8 * r, :] = gload[r] * gload[r]

    prepare(0)
    prepare(1)

    gate_d2d().wait_recv()
    gall[zh] = gall[4] + gdrecv[...]
    gate_copy(0).start()
    gate_copy(1).start()

    d2d(0).wait_recv()
    scale = round_up(chip_top(0))
    factors = [put_scale(way, 0, scale) for way in range(2)]
    for t in range(3):
        for way in range(2):
            z_piece(way, 0, t, chip_rows(0, t, way), factors[way])

    prepare(2)
    pl.semaphore_wait(known.at[0], 3)
    pl.semaphore_signal(known.at[1], inc=1, device_id=z_pair, device_id_type=MESH)

    tops = []
    for way in range(2):
        k = 1 + way
        d2d(k).wait_recv()
        tops.append(chip_top(k))
        factor = put_scale(way, 1, round_up(tops[way]))
        for t in range(3):
            z_piece(way, 1, t, chip_rows(k, t, 1 - way), factor)

    prepare(3)
    gate_copy(0).wait_recv()
    gate_copy(2).start()

    factors = []
    for t in range(3):
        for way in range(2):
            z_copy(way, 0, t).wait_recv()
            if t == 0:
                scale = round_up(tops[way] + z_scale(way, 0))
                factors.append(put_scale(way, 2, scale))
            values = chip_rows(1 + way, t, way) + z_values(way, 0, t)
            z_piece(way, 2, t, values, factors[way])

    gate_copy(1).wait_recv()
    gate_copy(2).wait_recv()
    gate_total = ((gall[0] + gall[1]) + gall[2]) + gall[3]
    gshard[...] = (gate_total * (1 / 16)).astype(BF16)

    def gate_send(i):
        return pltpu.make_async_remote_copy(
            src_ref=gshard, dst_ref=out_gate.at[:, pl.ds(pl.multiple_of(sa * 128, 128), 128)],
            send_sem=ga_sem.at[0], recv_sem=ga_sem.at[1],
            device_id=(row, (sa + i) % 32), device_id_type=MESH,
        )

    def gate_start(i, _):
        gate_send(i).start()
        return 0

    pl.semaphore_wait(known.at[1], 1)
    lax.fori_loop(1, 32, gate_start, 0)
    out_gate[:, pl.ds(pl.multiple_of(sa * 128, 128), 128)] = gshard[...]

    for t in range(3):
        part = squares[pl.ds(t * 128, 16, stride=8), :]
        for j in range(1, 8):
            part = part + squares[pl.ds(t * 128 + j, 16, stride=8), :]
        rowsums[16 * t : 16 * t + 16, :] = part
    rowsums[64:128, :] = jnp.zeros((64, 128), F32)
    norm_row = jnp.sum(rowsums[...].T, axis=0, keepdims=True)
    lane = lax.broadcasted_iota(jnp.int32, (1, 128), 1)

    def msg_send(piece, i):
        return pltpu.make_async_remote_copy(
            src_ref=msgs.at[piece, (sa + i) % 32], dst_ref=recv.at[piece, sa],
            send_sem=ms_sem.at[piece], recv_sem=mr_sem.at[piece],
            device_id=(row, (sa + i) % 32), device_id_type=MESH,
        )

    def send_all(piece):
        def start(i, _):
            msg_send(piece, i).start()
            return 0

        lax.fori_loop(1, 32, start, 0)
        recv[piece, sa] = msgs[piece, sa]

    d2d(3).wait_recv()
    for t in range(3):
        for half in range(2):
            total = chip_rows(3, t, half)
            z_copy(1 - half, 1, t).wait_recv()
            total = total + z_values(1 - half, 1, t)
            z_copy(half, 2, t).wait_recv()
            total = total + z_values(half, 2, t)
            served[t, 64 * half : 64 * half + 64, :] = (total * (1 / 16)).astype(BF16).astype(F32)
        final = served[t]
        square = jnp.sum(final * final, axis=(0, 1), keepdims=True)
        norm_row = jnp.where(lane == 64 + t, square, norm_row)
        if t == 1:
            for p in range(32):
                parts = [served[j, 4 * p : 4 * p + 4, :] for j in range(2)]
                msgs[0, p] = jnp.concatenate(parts, axis=0).astype(BF16)
            send_all(0)

    high = norm_row.astype(BF16).astype(F32)
    rest = norm_row - high
    middle = rest.astype(BF16).astype(F32)
    tail = jnp.concatenate([high, middle, rest - middle, jnp.zeros((1, 128), F32)], axis=0)
    for p in range(32):
        msgs[1, p] = jnp.concatenate([served[2, 4 * p : 4 * p + 4, :], tail], axis=0).astype(BF16)
    send_all(1)

    for k in range(4):
        d2d(k).wait_send()
    for way in range(2):
        for stage in range(3):
            for t in range(3):
                z_copy(way, stage, t).wait_send()
    gate_d2d().wait_send()
    for which in range(3):
        gate_copy(which).wait_send()
    others = out_gate.at[:, pl.ds(0, 31 * 128)]
    pltpu.make_async_copy(others, others, ga_sem.at[0]).wait()
    pltpu.make_async_copy(others, others, ga_sem.at[1]).wait()

    for piece in range(2):
        batch = recv.at[piece, pl.ds(0, 31)]
        pltpu.make_async_copy(batch, batch, ms_sem.at[piece]).wait()
        pltpu.make_async_copy(batch, batch, mr_sem.at[piece]).wait()


def unpack(recv, gates, out_w1, out_w3, out_w2, out_gate, out_soup, out_rep):
    row = lax.axis_index("row")
    routed = gates[...]
    out_gate[...] = routed
    wide = routed.astype(F32)
    mine = lax.broadcasted_iota(jnp.int32, wide.shape, 0) == row
    gate_square = jnp.sum(jnp.where(mine, wide * wide, 0.0), axis=(0, 1), keepdims=True)

    totals = jnp.zeros((4, 128), F32)
    for s in range(32):
        columns = slice(128 * s, 128 * s + 128)
        first = recv[0, s].astype(F32)
        last = recv[1, s].astype(F32)
        out_w1[0, :, columns] = first[0:4].astype(BF16)
        out_w3[0, :, columns] = first[4:8].astype(BF16)
        out_w2[0, :, columns] = last[0:4].astype(BF16)
        totals = totals + last[4:8]
    total_row = (totals[0:1] + totals[1:2]) + totals[2:3]

    lane = lax.broadcasted_iota(jnp.int32, (1, 128), 1)
    for r in range(2):
        for t in range(4):
            entries = pltpu.roll(total_row, 128 - (16 * t + 8 * r) if t + r else 0, 1)
            norms = jnp.sqrt(entries * (1 / (4096 if t == 3 else 524288)))
            out_rep[r, t : t + 1, :] = norms[:, 0:8]
    soup = pltpu.roll(total_row, 64, 1) * (1 / 524288)
    soup = jnp.sqrt(jnp.where(lane == 3, gate_square * (1 / 4096), soup))
    out_soup[...] = soup[:, 0:4]


def body(w1, w3, w2, gate):
    vmem = pl.BlockSpec(memory_space=pltpu.VMEM)
    hbm = pl.BlockSpec(memory_space=pl.ANY)
    dma = pltpu.SemaphoreType.DMA
    recv, gates = pl.pallas_call(
        kernel,
        name="soup",
        out_shape=(
            jax.ShapeDtypeStruct((2, 32, 8, 128), BF16),
            jax.ShapeDtypeStruct((8, 4096), BF16),
        ),
        in_specs=[hbm] * 4,
        out_specs=(vmem,) * 2,
        scratch_shapes=[
            pltpu.VMEM((4, 3, 2, 2, 128, 128), F32),
            pltpu.VMEM((2, 8, 128), F32),
            pltpu.VMEM((4, 392, 128), F32),
            pltpu.VMEM((4, 392, 128), F32),
            pltpu.VMEM((4, 392, 128), F32),
            pltpu.VMEM((384, 128), F32),
            pltpu.VMEM((128, 128), F32),
            pltpu.VMEM((2, 3, 208, 128), BF16),
            pltpu.VMEM((2, 3, 208, 128), BF16),
            pltpu.VMEM((5, 8, 128), F32),
            pltpu.VMEM((8, 128), F32),
            pltpu.VMEM((8, 128), BF16),
            pltpu.VMEM((3, 128, 128), F32),
            pltpu.VMEM((2, 32, 8, 128), BF16),
            dma((4, 3)),
            dma,
            dma((4,)),
            dma((4,)),
            dma((2, 3, 3)),
            dma((2, 3, 3)),
            dma((2,)),
            dma((2, 3)),
            dma((2,)),
            dma((2,)),
            dma((2,)),
            pltpu.SemaphoreType.REGULAR((2,)),
        ],
        compiler_params=pltpu.CompilerParams(collective_id=0, has_side_effects=True),
    )(w1, w3, w2, gate)
    outs = pl.pallas_call(
        unpack,
        name="unpack",
        out_shape=(
            jax.ShapeDtypeStruct((1, 4, 4096), BF16),
            jax.ShapeDtypeStruct((1, 4, 4096), BF16),
            jax.ShapeDtypeStruct((1, 4, 4096), BF16),
            jax.ShapeDtypeStruct((8, 4096), BF16),
            jax.ShapeDtypeStruct((1, 4), F32),
            jax.ShapeDtypeStruct((2, 4, 8), F32),
        ),
        in_specs=[vmem] * 2,
        out_specs=(vmem,) * 6,
    )(recv, gates)
    return (*outs[:5], outs[5].transpose(0, 2, 1))


def solution(mesh):
    in_specs = (
        P("row", None, None, "sa"),
        P("row", None, None, "sa"),
        P("row", None, None, "sa"),
        P("row", None, "sa"),
    )
    out_specs = (
        P("row", "sa", None),
        P("row", "sa", None),
        P("row", "sa", None),
        P(),
        P("row", None),
        P("row", None, None),
    )
    return jax.shard_map(body, mesh=mesh, in_specs=in_specs, out_specs=out_specs, check_vma=False)
```

```python
import functools

import jax
import jax.numpy as jnp
from jax import lax
from jax.experimental import pallas as pl
from jax.experimental.pallas import tpu as pltpu
from jax.sharding import PartitionSpec as P

MESH = pl.DeviceIdType.MESH
F32, BF16 = jnp.float32, jnp.bfloat16

SPAN = 2.0**7.875


def row_max(block8):
    return jnp.maximum(jnp.max(block8, axis=0, keepdims=True), 1e-30)


def round_up(scale):
    return (scale * 1.015625).astype(BF16)


def encoded(values, factor):
    u = values * factor
    u2 = u * u
    u4 = u2 * u2
    u8 = u4 * u4
    u16 = u8 * u8
    return jnp.where(u < 0, -u16, u16).astype(BF16)


def decoded(wire, factor):
    y = wire.astype(F32)
    root = lax.rsqrt(lax.rsqrt(lax.rsqrt(lax.rsqrt(jnp.abs(y)))))
    return jnp.where(y < 0, -root, root) * factor


def kernel(
    w1, w3, w2, gate,
    recv, out_gate,
    load, gload, sown, dsend, drecv, squares, rowsums,
    zsend, zrecv, gall, gdrecv, gshard, served, msgs,
    load_sem, gload_sem, ds_sem, dr_sem, zs_sem, zr_sem, gd_sem, gz_sem, ga_sem, ms_sem, mr_sem, known,
):
    weights = (w1, w3, w2)
    row, sa = lax.axis_index("row"), lax.axis_index("sa")
    zh, core = row // 2, row % 2
    partner = row + 1 - 2 * core
    up, down = (row + 2) % 8, (row + 6) % 8

    chips = [(zh + d) % 4 for d in (2, 1, 3, 0)]

    def load_copy(k, t):
        return pltpu.make_async_copy(
            weights[t].at[:, pl.ds(2 * chips[k], 2)], load.at[k, t], load_sem.at[k, t]
        )

    gate_load = pltpu.make_async_copy(gate, gload, gload_sem)
    gate_load.start()
    for t in range(3):
        load_copy(0, t).start()

    zl, x, y = sa // 16, (sa // 4) % 4, sa % 4
    x_line = [(row, zl * 16 + ((x + i) % 4) * 4 + y) for i in (1, 2, 3)]
    y_line = [(row, zl * 16 + x * 4 + (y + i) % 4) for i in (1, 2, 3)]
    z_pair = (row, sa + 16 - 32 * zl)
    barrier = pltpu.get_barrier_semaphore()
    for device in [(up, sa), (down, sa), (partner, sa), *x_line, *y_line, z_pair]:
        pl.semaphore_signal(barrier, inc=1, device_id=device, device_id_type=MESH)
    for k in range(1, 4):
        for t in range(3):
            load_copy(k, t).start()

    def chunk_sums(k, parity, dest):
        expert = 2 * chips[k] + parity
        top = jnp.zeros((8, 128), F32)
        for t in range(3):
            a, b = load[k, t, 0, parity], load[k, t, 1, parity]
            total = a + b
            dest[t * 128 : (t + 1) * 128, :] = total
            for r, v in ((0, a), (1, b)):
                index = pl.multiple_of((t * 16 + r * 8 + expert) * 8, 8)
                squares[pl.ds(index, 8), :] = jnp.sum((v * v).reshape(16, 8, 128), axis=0)
            if k < 3:
                top = jnp.maximum(top, jnp.max(jnp.abs(total).reshape(16, 8, 128), axis=0))
        if k < 3:
            dest[384:392, :] = top

    def d2d(k):
        return pltpu.make_async_remote_copy(
            src_ref=dsend.at[k], dst_ref=drecv.at[k], send_sem=ds_sem.at[k], recv_sem=dr_sem.at[k],
            device_id=(partner, sa), device_id_type=MESH,
        )

    def z_copy(way, stage, piece):
        rows = pl.ds(0, 80) if piece == 0 else pl.ds(16 + 64 * piece, 64)
        return pltpu.make_async_remote_copy(
            src_ref=zsend.at[way, stage, rows], dst_ref=zrecv.at[way, stage, rows],
            send_sem=zs_sem.at[way, stage, piece], recv_sem=zr_sem.at[way, stage, piece],
            device_id=((up, down)[way], sa), device_id_type=MESH,
        )

    def chip_rows(k, t, half):
        rows = slice(t * 128 + half * 64, t * 128 + half * 64 + 64)
        return sown[k, rows, :] + drecv[k, rows, :]

    def chip_top(k):
        return row_max(sown[k, 384:392, :] + drecv[k, 384:392, :])

    def put_scale(way, stage, scale):
        zsend[way, stage, 0:16, :] = jnp.broadcast_to(scale, (16, 128))
        return SPAN / scale.astype(F32)

    def z_piece(way, stage, t, values, factor):
        zsend[way, stage, 16 + 64 * t : 80 + 64 * t, :] = encoded(values, factor)
        z_copy(way, stage, t).start()

    def z_scale(way, stage):
        return zrecv[way, stage, 0:16, :].astype(F32)[0:1]

    def z_values(way, stage, t):
        return decoded(
            zrecv[way, stage, 16 + 64 * t : 80 + 64 * t, :], z_scale(way, stage) * (1 / SPAN)
        )

    def prepare(k):
        for t in range(3):
            load_copy(k, t).wait()
        chunk_sums(k, 1 - core, dsend.at[k])
        if k == 0:
            pl.semaphore_wait(barrier, 10)
            gate_d2d().start()
        d2d(k).start()
        if k == 0:
            for device in x_line:
                pl.semaphore_signal(known.at[0], inc=1, device_id=device, device_id_type=MESH)
        chunk_sums(k, core, sown.at[k])

    def gate_d2d():
        return pltpu.make_async_remote_copy(
            src_ref=gall.at[4], dst_ref=gdrecv, send_sem=gd_sem.at[0], recv_sem=gd_sem.at[1],
            device_id=(partner, sa), device_id_type=MESH,
        )

    def gate_copy(which):
        slot = (zh, zh, (zh + 3) % 4)[which]
        return pltpu.make_async_remote_copy(
            src_ref=gall.at[slot], dst_ref=gall.at[slot],
            send_sem=gz_sem.at[0, which], recv_sem=gz_sem.at[1, which],
            device_id=((up, down, up)[which], sa), device_id_type=MESH,
        )

    gate_load.wait()
    gall[4] = gload[0] + gload[1]
    for r in range(2):
        rowsums[48 + 8 * r : 56 + 8 * r, :] = gload[r] * gload[r]

    prepare(0)
    prepare(1)

    gate_d2d().wait_recv()
    gall[zh] = gall[4] + gdrecv[...]
    gate_copy(0).start()
    gate_copy(1).start()

    d2d(0).wait_recv()
    scale = round_up(chip_top(0))
    factors = [put_scale(way, 0, scale) for way in range(2)]
    for t in range(3):
        for way in range(2):
            z_piece(way, 0, t, chip_rows(0, t, way), factors[way])

    prepare(2)
    pl.semaphore_wait(known.at[0], 3)
    pl.semaphore_signal(known.at[1], inc=1, device_id=z_pair, device_id_type=MESH)

    tops = []
    for way in range(2):
        k = 1 + way
        d2d(k).wait_recv()
        tops.append(chip_top(k))
        factor = put_scale(way, 1, round_up(tops[way]))
        for t in range(3):
            z_piece(way, 1, t, chip_rows(k, t, 1 - way), factor)

    prepare(3)
    gate_copy(0).wait_recv()
    gate_copy(2).start()

    factors = []
    for t in range(3):
        for way in range(2):
            z_copy(way, 0, t).wait_recv()
            if t == 0:
                scale = round_up(tops[way] + z_scale(way, 0))
                factors.append(put_scale(way, 2, scale))
            values = chip_rows(1 + way, t, way) + z_values(way, 0, t)
            z_piece(way, 2, t, values, factors[way])

    gate_copy(1).wait_recv()
    gate_copy(2).wait_recv()
    gate_total = ((gall[0] + gall[1]) + gall[2]) + gall[3]
    gshard[...] = (gate_total * (1 / 16)).astype(BF16)

    def gate_send(i):
        return pltpu.make_async_remote_copy(
            src_ref=gshard, dst_ref=out_gate.at[:, pl.ds(pl.multiple_of(sa * 128, 128), 128)],
            send_sem=ga_sem.at[0], recv_sem=ga_sem.at[1],
            device_id=(row, (sa + i) % 32), device_id_type=MESH,
        )

    def gate_start(i, _):
        gate_send(i).start()
        return 0

    pl.semaphore_wait(known.at[1], 1)
    lax.fori_loop(1, 32, gate_start, 0)
    out_gate[:, pl.ds(pl.multiple_of(sa * 128, 128), 128)] = gshard[...]

    for t in range(3):
        part = squares[pl.ds(t * 128, 16, stride=8), :]
        for j in range(1, 8):
            part = part + squares[pl.ds(t * 128 + j, 16, stride=8), :]
        rowsums[16 * t : 16 * t + 16, :] = part
    rowsums[64:128, :] = jnp.zeros((64, 128), F32)
    norm_row = jnp.sum(rowsums[...].T, axis=0, keepdims=True)
    lane = lax.broadcasted_iota(jnp.int32, (1, 128), 1)

    def msg_send(piece, i):
        return pltpu.make_async_remote_copy(
            src_ref=msgs.at[piece, (sa + i) % 32], dst_ref=recv.at[piece, sa],
            send_sem=ms_sem.at[piece], recv_sem=mr_sem.at[piece],
            device_id=(row, (sa + i) % 32), device_id_type=MESH,
        )

    def send_all(piece):
        def start(i, _):
            msg_send(piece, i).start()
            return 0

        lax.fori_loop(1, 32, start, 0)
        recv[piece, sa] = msgs[piece, sa]

    d2d(3).wait_recv()
    for t in range(3):
        for half in range(2):
            total = chip_rows(3, t, half)
            z_copy(1 - half, 1, t).wait_recv()
            total = total + z_values(1 - half, 1, t)
            z_copy(half, 2, t).wait_recv()
            total = total + z_values(half, 2, t)
            served[t, 64 * half : 64 * half + 64, :] = (total * (1 / 16)).astype(BF16).astype(F32)
        final = served[t]
        square = jnp.sum(final * final, axis=(0, 1), keepdims=True)
        norm_row = jnp.where(lane == 64 + t, square, norm_row)
        if t == 1:
            for p in range(32):
                parts = [served[j, 4 * p : 4 * p + 4, :] for j in range(2)]
                msgs[0, p] = jnp.concatenate(parts, axis=0).astype(BF16)
            send_all(0)

    high = norm_row.astype(BF16).astype(F32)
    rest = norm_row - high
    middle = rest.astype(BF16).astype(F32)
    tail = jnp.concatenate([high, middle, rest - middle, jnp.zeros((1, 128), F32)], axis=0)
    for p in range(32):
        msgs[1, p] = jnp.concatenate([served[2, 4 * p : 4 * p + 4, :], tail], axis=0).astype(BF16)
    send_all(1)

    for k in range(4):
        d2d(k).wait_send()
    for way in range(2):
        for stage in range(3):
            for t in range(3):
                z_copy(way, stage, t).wait_send()
    gate_d2d().wait_send()
    for which in range(3):
        gate_copy(which).wait_send()
    others = out_gate.at[:, pl.ds(0, 31 * 128)]
    pltpu.make_async_copy(others, others, ga_sem.at[0]).wait()
    pltpu.make_async_copy(others, others, ga_sem.at[1]).wait()

    for piece in range(2):
        batch = recv.at[piece, pl.ds(0, 31)]
        pltpu.make_async_copy(batch, batch, ms_sem.at[piece]).wait()
        pltpu.make_async_copy(batch, batch, mr_sem.at[piece]).wait()


def unpack(recv, gates, out_w1, out_w3, out_w2, out_gate, out_soup, out_rep):
    row = lax.axis_index("row")
    routed = gates[...]
    out_gate[...] = routed
    wide = routed.astype(F32)
    mine = lax.broadcasted_iota(jnp.int32, wide.shape, 0) == row
    gate_square = jnp.sum(jnp.where(mine, wide * wide, 0.0), axis=(0, 1), keepdims=True)

    totals = jnp.zeros((4, 128), F32)
    for s in range(32):
        columns = slice(128 * s, 128 * s + 128)
        first = recv[0, s].astype(F32)
        last = recv[1, s].astype(F32)
        out_w1[0, :, columns] = first[0:4].astype(BF16)
        out_w3[0, :, columns] = first[4:8].astype(BF16)
        out_w2[0, :, columns] = last[0:4].astype(BF16)
        totals = totals + last[4:8]
    total_row = (totals[0:1] + totals[1:2]) + totals[2:3]

    lane = lax.broadcasted_iota(jnp.int32, (1, 128), 1)
    for r in range(2):
        for t in range(4):
            entries = pltpu.roll(total_row, 128 - (16 * t + 8 * r) if t + r else 0, 1)
            norms = jnp.sqrt(entries * (1 / (4096 if t == 3 else 524288)))
            out_rep[r, t : t + 1, :] = norms[:, 0:8]
    soup = pltpu.roll(total_row, 64, 1) * (1 / 524288)
    soup = jnp.sqrt(jnp.where(lane == 3, gate_square * (1 / 4096), soup))
    out_soup[...] = soup[:, 0:4]


def body(w1, w3, w2, gate):
    vmem = pl.BlockSpec(memory_space=pltpu.VMEM)
    hbm = pl.BlockSpec(memory_space=pl.ANY)
    dma = pltpu.SemaphoreType.DMA
    recv, gates = pl.pallas_call(
        kernel,
        name="soup",
        out_shape=(
            pltpu.VMEM((2, 32, 8, 128), BF16),
            pltpu.VMEM((8, 4096), BF16),
        ),
        in_specs=[hbm] * 4,
        out_specs=(vmem,) * 2,
        scratch_shapes=[
            pltpu.VMEM((4, 3, 2, 2, 128, 128), F32),
            pltpu.VMEM((2, 8, 128), F32),
            pltpu.VMEM((4, 392, 128), F32),
            pltpu.VMEM((4, 392, 128), F32),
            pltpu.VMEM((4, 392, 128), F32),
            pltpu.VMEM((384, 128), F32),
            pltpu.VMEM((128, 128), F32),
            pltpu.VMEM((2, 3, 208, 128), BF16),
            pltpu.VMEM((2, 3, 208, 128), BF16),
            pltpu.VMEM((5, 8, 128), F32),
            pltpu.VMEM((8, 128), F32),
            pltpu.VMEM((8, 128), BF16),
            pltpu.VMEM((3, 128, 128), F32),
            pltpu.VMEM((2, 32, 8, 128), BF16),
            dma((4, 3)),
            dma,
            dma((4,)),
            dma((4,)),
            dma((2, 3, 3)),
            dma((2, 3, 3)),
            dma((2,)),
            dma((2, 3)),
            dma((2,)),
            dma((2,)),
            dma((2,)),
            pltpu.SemaphoreType.REGULAR((2,)),
        ],
        compiler_params=pltpu.CompilerParams(collective_id=0, has_side_effects=True, vmem_limit_bytes=56 * 2**20),
    )(w1, w3, w2, gate)
    outs = pl.pallas_call(
        unpack,
        name="unpack",
        out_shape=(
            jax.ShapeDtypeStruct((1, 4, 4096), BF16),
            jax.ShapeDtypeStruct((1, 4, 4096), BF16),
            jax.ShapeDtypeStruct((1, 4, 4096), BF16),
            jax.ShapeDtypeStruct((8, 4096), BF16),
            jax.ShapeDtypeStruct((1, 4), F32),
            jax.ShapeDtypeStruct((2, 4, 8), F32),
        ),
        in_specs=[vmem] * 2,
        out_specs=(vmem,) * 6,
        compiler_params=pltpu.CompilerParams(vmem_limit_bytes=4 * 2**20),
    )(recv, gates)
    return (*outs[:5], outs[5].transpose(0, 2, 1))


def solution(mesh):
    in_specs = (
        P("row", None, None, "sa"),
        P("row", None, None, "sa"),
        P("row", None, None, "sa"),
        P("row", None, "sa"),
    )
    out_specs = (
        P("row", "sa", None),
        P("row", "sa", None),
        P("row", "sa", None),
        P(),
        P("row", None),
        P("row", None, None),
    )
    return jax.shard_map(body, mesh=mesh, in_specs=in_specs, out_specs=out_specs, check_vma=False)
```

```python
import functools

import jax
import jax.numpy as jnp
from jax import lax
from jax.experimental import pallas as pl
from jax.experimental.pallas import tpu as pltpu
from jax.sharding import PartitionSpec as P

MESH = pl.DeviceIdType.MESH
F32, BF16 = jnp.float32, jnp.bfloat16

SPAN = 2.0**7.875


STEPS = sorted(
    [(dz, dx, dy) for dz in (0, 1) for dx in range(4) for dy in range(4) if dz + dx + dy],
    key=lambda d: -(d[0] + min(d[1], 4 - d[1]) + min(d[2], 4 - d[2])),
)
FIRST, BLOCK = 8, 32


def row_max(block8):
    return jnp.maximum(jnp.max(block8, axis=0, keepdims=True), 1e-30)


def round_up(scale):
    return (scale * 1.015625).astype(BF16)


def encoded(values, factor):
    u = values * factor
    u2 = u * u
    u4 = u2 * u2
    u8 = u4 * u4
    u16 = u8 * u8
    return jnp.where(u < 0, -u16, u16).astype(BF16)


def decoded(wire, factor):
    y = wire.astype(F32)
    root = lax.rsqrt(lax.rsqrt(lax.rsqrt(lax.rsqrt(jnp.abs(y)))))
    return jnp.where(y < 0, -root, root) * factor


def kernel(
    w1, w3, w2, gate,
    recv, out_gate,
    load, gload, sown, dsend, drecv, squares, rowsums,
    zsend, zrecv, gall, gdrecv, gshard, served, msgs,
    load_sem, gload_sem, ds_sem, dr_sem, zs_sem, zr_sem, gd_sem, gz_sem, ga_sem, ms_sem, mr_sem, known,
):
    weights = (w1, w3, w2)
    row, sa = lax.axis_index("row"), lax.axis_index("sa")
    zh, core = row // 2, row % 2
    partner = row + 1 - 2 * core
    up, down = (row + 2) % 8, (row + 6) % 8

    chips = [(zh + d) % 4 for d in (2, 1, 3, 0)]

    def load_copy(k, t):
        return pltpu.make_async_copy(
            weights[t].at[:, pl.ds(2 * chips[k], 2)], load.at[k, t], load_sem.at[k, t]
        )

    gate_load = pltpu.make_async_copy(gate, gload, gload_sem)
    gate_load.start()
    for t in range(3):
        load_copy(0, t).start()

    zl, x, y = sa // 16, (sa // 4) % 4, sa % 4
    zs, xs, ys = [zl * 16, 16 - zl * 16], [((x + i) % 4) * 4 for i in range(4)], [(y + i) % 4 for i in range(4)]
    x_line = [(row, zs[0] + xs[i] + y) for i in (1, 2, 3)]
    y_line = [(row, zs[0] + xs[0] + ys[i]) for i in (1, 2, 3)]
    z_pair = (row, zs[1] + xs[0] + y)
    sa_peers = [zs[dz] + xs[dx] + ys[dy] for dz, dx, dy in STEPS]
    barrier = pltpu.get_barrier_semaphore()
    for device in [(up, sa), (down, sa), (partner, sa), *x_line, *y_line, z_pair]:
        pl.semaphore_signal(barrier, inc=1, device_id=device, device_id_type=MESH)
    for k in range(1, 4):
        for t in range(3):
            load_copy(k, t).start()

    def chunk_sums(k, parity, dest):
        expert = 2 * chips[k] + parity
        top = jnp.zeros((8, 128), F32)
        for t in range(3):
            a, b = load[k, t, 0, parity], load[k, t, 1, parity]
            total = a + b
            dest[t * 128 : (t + 1) * 128, :] = total
            for r, v in ((0, a), (1, b)):
                index = pl.multiple_of((t * 16 + r * 8 + expert) * 8, 8)
                squares[pl.ds(index, 8), :] = jnp.sum((v * v).reshape(16, 8, 128), axis=0)
            if k < 3:
                top = jnp.maximum(top, jnp.max(jnp.abs(total).reshape(16, 8, 128), axis=0))
        if k < 3:
            dest[384:392, :] = top

    def d2d(k):
        return pltpu.make_async_remote_copy(
            src_ref=dsend.at[k], dst_ref=drecv.at[k], send_sem=ds_sem.at[k], recv_sem=dr_sem.at[k],
            device_id=(partner, sa), device_id_type=MESH,
        )

    def z_copy(way, stage, piece):
        if stage == 1:
            rows = pl.ds(0, FIRST + 192)
        elif piece == 0:
            rows = pl.ds(0, FIRST + BLOCK)
        else:
            rows = pl.ds(FIRST + BLOCK * piece, BLOCK)
        return pltpu.make_async_remote_copy(
            src_ref=zsend.at[way, stage, rows], dst_ref=zrecv.at[way, stage, rows],
            send_sem=zs_sem.at[way, stage, piece], recv_sem=zr_sem.at[way, stage, piece],
            device_id=((up, down)[way], sa), device_id_type=MESH,
        )

    def chip_rows(k, piece, half):
        t, part = piece // 2, piece % 2
        start = t * 128 + half * 64 + part * BLOCK
        return sown[k, start : start + BLOCK, :] + drecv[k, start : start + BLOCK, :]

    def chip_top(k):
        return row_max(sown[k, 384:392, :] + drecv[k, 384:392, :])

    def put_scale(way, stage, scale):
        zsend[way, stage, 0:FIRST, :] = jnp.broadcast_to(scale, (FIRST, 128))
        return SPAN / scale.astype(F32)

    def block(piece):
        return slice(FIRST + BLOCK * piece, FIRST + BLOCK * piece + BLOCK)

    def z_scale(way, stage):
        return zrecv[way, stage, 0:FIRST, :].astype(F32)[0:1]

    def z_values(way, stage, piece):
        return decoded(zrecv[way, stage, block(piece), :], z_scale(way, stage) * (1 / SPAN))

    def prepare(k):
        for t in range(3):
            load_copy(k, t).wait()
        chunk_sums(k, 1 - core, dsend.at[k])
        if k == 0:
            pl.semaphore_wait(barrier, 10)
            gate_d2d().start()
        d2d(k).start()
        if k == 0:
            pl.semaphore_signal(known.at[2], inc=1, device_id=(up, sa), device_id_type=MESH)
            for device in x_line:
                pl.semaphore_signal(known.at[0], inc=1, device_id=device, device_id_type=MESH)
        chunk_sums(k, core, sown.at[k])

    def gate_d2d():
        return pltpu.make_async_remote_copy(
            src_ref=gall.at[4], dst_ref=gdrecv, send_sem=gd_sem.at[0], recv_sem=gd_sem.at[1],
            device_id=(partner, sa), device_id_type=MESH,
        )

    def gate_copy(which):
        return pltpu.make_async_remote_copy(
            src_ref=gall.at[zh], dst_ref=gall.at[zh],
            send_sem=gz_sem.at[0, which], recv_sem=gz_sem.at[1, which],
            device_id=((up, down, (row + 4) % 8)[which], sa), device_id_type=MESH,
        )

    gate_load.wait()
    gall[4] = gload[0] + gload[1]
    for r in range(2):
        rowsums[48 + 8 * r : 56 + 8 * r, :] = gload[r] * gload[r]

    prepare(0)
    prepare(1)

    gate_d2d().wait_recv()
    gall[zh] = gall[4] + gdrecv[...]
    pl.semaphore_wait(known.at[2], 1)
    for which in (2, 0, 1):
        gate_copy(which).start()

    d2d(0).wait_recv()
    scale = round_up(chip_top(0))
    factors = [put_scale(way, 0, scale) for way in range(2)]
    for piece in range(6):
        for way in range(2):
            zsend[way, 0, block(piece), :] = encoded(chip_rows(0, piece, way), factors[way])
            z_copy(way, 0, piece).start()

    prepare(2)
    pl.semaphore_wait(known.at[0], 3)
    pl.semaphore_signal(known.at[1], inc=1, device_id=z_pair, device_id_type=MESH)

    tops = []
    for way in range(2):
        k = 1 + way
        d2d(k).wait_recv()
        tops.append(chip_top(k))
        factor = put_scale(way, 1, round_up(tops[way]))
        for piece in range(6):
            zsend[way, 1, block(piece), :] = encoded(chip_rows(k, piece, 1 - way), factor)
        z_copy(way, 1, 0).start()

    prepare(3)

    factors = []
    for piece in range(6):
        for way in range(2):
            z_copy(way, 0, piece).wait_recv()
            if piece == 0:
                scale = round_up(tops[way] + z_scale(way, 0))
                factors.append(put_scale(way, 2, scale))
            values = chip_rows(1 + way, piece, way) + z_values(way, 0, piece)
            zsend[way, 2, block(piece), :] = encoded(values, factors[way])
            z_copy(way, 2, piece).start()

    for which in range(3):
        gate_copy(which).wait_recv()
    gate_total = ((gall[0] + gall[1]) + gall[2]) + gall[3]
    gshard[...] = (gate_total * (1 / 16)).astype(BF16)

    pl.semaphore_wait(known.at[1], 1)
    for peer in sa_peers:
        pltpu.make_async_remote_copy(
            src_ref=gshard, dst_ref=out_gate.at[:, pl.ds(pl.multiple_of(sa * 128, 128), 128)],
            send_sem=ga_sem.at[0], recv_sem=ga_sem.at[1],
            device_id=(row, peer), device_id_type=MESH,
        ).start()
    out_gate[:, pl.ds(pl.multiple_of(sa * 128, 128), 128)] = gshard[...]

    for t in range(3):
        part = squares[pl.ds(t * 128, 16, stride=8), :]
        for j in range(1, 8):
            part = part + squares[pl.ds(t * 128 + j, 16, stride=8), :]
        rowsums[16 * t : 16 * t + 16, :] = part
    rowsums[64:128, :] = jnp.zeros((64, 128), F32)
    norm_row = jnp.sum(rowsums[...].T, axis=0, keepdims=True)
    lane = lax.broadcasted_iota(jnp.int32, (1, 128), 1)

    def send_all(piece):
        for peer in sa_peers:
            pltpu.make_async_remote_copy(
                src_ref=msgs.at[piece, peer], dst_ref=recv.at[piece, sa],
                send_sem=ms_sem.at[piece], recv_sem=mr_sem.at[piece],
                device_id=(row, peer), device_id_type=MESH,
            ).start()
        recv[piece, sa] = msgs[piece, sa]

    d2d(3).wait_recv()
    for way in range(2):
        z_copy(way, 1, 0).wait_recv()
    for t in range(3):
        for part in range(2):
            for half in range(2):
                piece = 2 * t + part
                total = chip_rows(3, piece, half) + z_values(1 - half, 1, piece)
                z_copy(half, 2, piece).wait_recv()
                total = total + z_values(half, 2, piece)
                start = 64 * half + BLOCK * part
                served[t, start : start + BLOCK, :] = (total * (1 / 16)).astype(BF16).astype(F32)
        final = served[t]
        square = jnp.sum(final * final, axis=(0, 1), keepdims=True)
        norm_row = jnp.where(lane == 64 + t, square, norm_row)
        if t == 1:
            for p in range(32):
                parts = [served[j, 4 * p : 4 * p + 4, :] for j in range(2)]
                msgs[0, p] = jnp.concatenate(parts, axis=0).astype(BF16)
            send_all(0)

    high = norm_row.astype(BF16).astype(F32)
    rest = norm_row - high
    middle = rest.astype(BF16).astype(F32)
    tail = jnp.concatenate([high, middle, rest - middle, jnp.zeros((1, 128), F32)], axis=0)
    for p in range(32):
        msgs[1, p] = jnp.concatenate([served[2, 4 * p : 4 * p + 4, :], tail], axis=0).astype(BF16)
    send_all(1)

    for k in range(4):
        d2d(k).wait_send()
    for way in range(2):
        z_copy(way, 1, 0).wait_send()
        for stage in (0, 2):
            for piece in range(6):
                z_copy(way, stage, piece).wait_send()
    gate_d2d().wait_send()
    for which in range(3):
        gate_copy(which).wait_send()
    others = out_gate.at[:, pl.ds(0, 31 * 128)]
    pltpu.make_async_copy(others, others, ga_sem.at[0]).wait()
    pltpu.make_async_copy(others, others, ga_sem.at[1]).wait()

    for piece in range(2):
        batch = recv.at[piece, pl.ds(0, 31)]
        pltpu.make_async_copy(batch, batch, ms_sem.at[piece]).wait()
        pltpu.make_async_copy(batch, batch, mr_sem.at[piece]).wait()


def unpack(recv, gates, out_w1, out_w3, out_w2, out_gate, out_soup, out_rep):
    row = lax.axis_index("row")
    routed = gates[...]
    out_gate[...] = routed
    wide = routed.astype(F32)
    mine = lax.broadcasted_iota(jnp.int32, wide.shape, 0) == row
    gate_square = jnp.sum(jnp.where(mine, wide * wide, 0.0), axis=(0, 1), keepdims=True)

    totals = jnp.zeros((4, 128), F32)
    for s in range(32):
        columns = slice(128 * s, 128 * s + 128)
        first = recv[0, s].astype(F32)
        last = recv[1, s].astype(F32)
        out_w1[0, :, columns] = first[0:4].astype(BF16)
        out_w3[0, :, columns] = first[4:8].astype(BF16)
        out_w2[0, :, columns] = last[0:4].astype(BF16)
        totals = totals + last[4:8]
    total_row = (totals[0:1] + totals[1:2]) + totals[2:3]

    lane = lax.broadcasted_iota(jnp.int32, (1, 128), 1)
    for r in range(2):
        for t in range(4):
            entries = pltpu.roll(total_row, 128 - (16 * t + 8 * r) if t + r else 0, 1)
            norms = jnp.sqrt(entries * (1 / (4096 if t == 3 else 524288)))
            out_rep[r, t : t + 1, :] = norms[:, 0:8]
    soup = pltpu.roll(total_row, 64, 1) * (1 / 524288)
    soup = jnp.sqrt(jnp.where(lane == 3, gate_square * (1 / 4096), soup))
    out_soup[...] = soup[:, 0:4]


def body(w1, w3, w2, gate):
    vmem = pl.BlockSpec(memory_space=pltpu.VMEM)
    hbm = pl.BlockSpec(memory_space=pl.ANY)
    dma = pltpu.SemaphoreType.DMA
    recv, gates = pl.pallas_call(
        kernel,
        name="soup",
        out_shape=(
            pltpu.VMEM((2, 32, 8, 128), BF16),
            pltpu.VMEM((8, 4096), BF16),
        ),
        in_specs=[hbm] * 4,
        out_specs=(vmem,) * 2,
        scratch_shapes=[
            pltpu.VMEM((4, 3, 2, 2, 128, 128), F32),
            pltpu.VMEM((2, 8, 128), F32),
            pltpu.VMEM((4, 392, 128), F32),
            pltpu.VMEM((4, 392, 128), F32),
            pltpu.VMEM((4, 392, 128), F32),
            pltpu.VMEM((384, 128), F32),
            pltpu.VMEM((128, 128), F32),
            pltpu.VMEM((2, 3, FIRST + 192, 128), BF16),
            pltpu.VMEM((2, 3, FIRST + 192, 128), BF16),
            pltpu.VMEM((5, 8, 128), F32),
            pltpu.VMEM((8, 128), F32),
            pltpu.VMEM((8, 128), BF16),
            pltpu.VMEM((3, 128, 128), F32),
            pltpu.VMEM((2, 32, 8, 128), BF16),
            dma((4, 3)),
            dma,
            dma((4,)),
            dma((4,)),
            dma((2, 3, 6)),
            dma((2, 3, 6)),
            dma((2,)),
            dma((2, 3)),
            dma((2,)),
            dma((2,)),
            dma((2,)),
            pltpu.SemaphoreType.REGULAR((3,)),
        ],
        compiler_params=pltpu.CompilerParams(collective_id=0, has_side_effects=True, vmem_limit_bytes=56 * 2**20),
    )(w1, w3, w2, gate)
    outs = pl.pallas_call(
        unpack,
        name="unpack",
        out_shape=(
            jax.ShapeDtypeStruct((1, 4, 4096), BF16),
            jax.ShapeDtypeStruct((1, 4, 4096), BF16),
            jax.ShapeDtypeStruct((1, 4, 4096), BF16),
            jax.ShapeDtypeStruct((8, 4096), BF16),
            jax.ShapeDtypeStruct((1, 4), F32),
            jax.ShapeDtypeStruct((2, 4, 8), F32),
        ),
        in_specs=[vmem] * 2,
        out_specs=(vmem,) * 6,
        compiler_params=pltpu.CompilerParams(vmem_limit_bytes=4 * 2**20),
    )(recv, gates)
    return (*outs[:5], outs[5].transpose(0, 2, 1))


def solution(mesh):
    in_specs = (
        P("row", None, None, "sa"),
        P("row", None, None, "sa"),
        P("row", None, None, "sa"),
        P("row", None, "sa"),
    )
    out_specs = (
        P("row", "sa", None),
        P("row", "sa", None),
        P("row", "sa", None),
        P(),
        P("row", None),
        P("row", None, None),
    )
    return jax.shard_map(body, mesh=mesh, in_specs=in_specs, out_specs=out_specs, check_vma=False)
```

```python
import functools

import jax
import jax.numpy as jnp
from jax import lax
from jax.experimental import pallas as pl
from jax.experimental.pallas import tpu as pltpu
from jax.sharding import PartitionSpec as P

MESH = pl.DeviceIdType.MESH
F32, BF16 = jnp.float32, jnp.bfloat16

SPAN = 2.0**7.875


STEPS = sorted(
    [(dz, dx, dy) for dz in (0, 1) for dx in range(4) for dy in range(4) if dz + dx + dy],
    key=lambda d: -(d[0] + min(d[1], 4 - d[1]) + min(d[2], 4 - d[2])),
)
FIRST, BLOCK = 8, 32


def row_max(block8):
    return jnp.maximum(jnp.max(block8, axis=0, keepdims=True), 1e-30)


def round_up(scale):
    return (scale * 1.015625).astype(BF16)


def encoded(values, factor):
    u = values * factor
    u2 = u * u
    u4 = u2 * u2
    u8 = u4 * u4
    u16 = u8 * u8
    return jnp.where(u < 0, -u16, u16).astype(BF16)


def decoded(wire, factor):
    y = wire.astype(F32)
    root = lax.rsqrt(lax.rsqrt(lax.rsqrt(lax.rsqrt(jnp.abs(y)))))
    return jnp.where(y < 0, -root, root) * factor


def kernel(
    w1, w3, w2, gate,
    recv, out_gate,
    load, gload, sown, dsend, drecv, squares, rowsums,
    zsend, zrecv, gall, gdrecv, gshard, served, msgs,
    load_sem, gload_sem, ds_sem, dr_sem, zs_sem, zr_sem, gd_sem, gz_sem, ga_sem, ms_sem, mr_sem, known,
):
    weights = (w1, w3, w2)
    row, sa = lax.axis_index("row"), lax.axis_index("sa")
    zh, core = row // 2, row % 2
    partner = row + 1 - 2 * core
    up, down = (row + 2) % 8, (row + 6) % 8

    chips = [(zh + d) % 4 for d in (2, 1, 3, 0)]

    def load_copy(k, t):
        return pltpu.make_async_copy(
            weights[t].at[:, pl.ds(2 * chips[k], 2)], load.at[k, t], load_sem.at[k, t]
        )

    gate_load = pltpu.make_async_copy(gate, gload, gload_sem)
    gate_load.start()
    for t in range(3):
        load_copy(0, t).start()

    zl, x, y = sa // 16, (sa // 4) % 4, sa % 4
    zs, xs, ys = [zl * 16, 16 - zl * 16], [((x + i) % 4) * 4 for i in range(4)], [(y + i) % 4 for i in range(4)]
    x_line = [(row, zs[0] + xs[i] + y) for i in (1, 2, 3)]
    y_line = [(row, zs[0] + xs[0] + ys[i]) for i in (1, 2, 3)]
    z_pair = (row, zs[1] + xs[0] + y)
    sa_peers = [zs[dz] + xs[dx] + ys[dy] for dz, dx, dy in STEPS]
    barrier = pltpu.get_barrier_semaphore()
    for device in [(up, sa), (down, sa), (partner, sa), *x_line, *y_line, z_pair]:
        pl.semaphore_signal(barrier, inc=1, device_id=device, device_id_type=MESH)
    for k in range(1, 4):
        for t in range(3):
            load_copy(k, t).start()

    def chunk_sums(k, parity, dest):
        expert = 2 * chips[k] + parity
        top = jnp.zeros((8, 128), F32)
        for t in range(3):
            a, b = load[k, t, 0, parity], load[k, t, 1, parity]
            total = a + b
            dest[t * 128 : (t + 1) * 128, :] = total
            for r, v in ((0, a), (1, b)):
                index = pl.multiple_of((t * 16 + r * 8 + expert) * 8, 8)
                squares[pl.ds(index, 8), :] = jnp.sum((v * v).reshape(16, 8, 128), axis=0)
            if k < 3:
                top = jnp.maximum(top, jnp.max(jnp.abs(total).reshape(16, 8, 128), axis=0))
        if k < 3:
            dest[384:392, :] = top

    def d2d(k):
        return pltpu.make_async_remote_copy(
            src_ref=dsend.at[k], dst_ref=drecv.at[k], send_sem=ds_sem.at[k], recv_sem=dr_sem.at[k],
            device_id=(partner, sa), device_id_type=MESH,
        )

    def z_copy(way, stage, piece):
        if stage == 1:
            rows = pl.ds(0, FIRST + 192)
        elif piece == 0:
            rows = pl.ds(0, FIRST + BLOCK)
        else:
            rows = pl.ds(FIRST + BLOCK * piece, BLOCK)
        return pltpu.make_async_remote_copy(
            src_ref=zsend.at[way, stage, rows], dst_ref=zrecv.at[way, stage, rows],
            send_sem=zs_sem.at[way, stage, piece], recv_sem=zr_sem.at[way, stage, piece],
            device_id=((up, down)[way], sa), device_id_type=MESH,
        )

    def chip_rows(k, piece, half):
        t, part = piece // 2, piece % 2
        start = t * 128 + half * 64 + part * BLOCK
        return sown[k, start : start + BLOCK, :] + drecv[k, start : start + BLOCK, :]

    def chip_top(k):
        return row_max(sown[k, 384:392, :] + drecv[k, 384:392, :])

    def put_scale(way, stage, scale):
        zsend[way, stage, 0:FIRST, :] = jnp.broadcast_to(scale, (FIRST, 128))
        return SPAN / scale.astype(F32)

    def block(piece):
        return slice(FIRST + BLOCK * piece, FIRST + BLOCK * piece + BLOCK)

    def z_scale(way, stage):
        return zrecv[way, stage, 0:FIRST, :].astype(F32)[0:1]

    def z_values(way, stage, piece):
        return decoded(zrecv[way, stage, block(piece), :], z_scale(way, stage) * (1 / SPAN))

    def prepare(k):
        for t in range(3):
            load_copy(k, t).wait()
        chunk_sums(k, 1 - core, dsend.at[k])
        if k == 0:
            pl.semaphore_wait(barrier, 10)
        d2d(k).start()
        if k == 0:

            @pl.when(core == 0)
            def _():
                gate_d2d().start()

            pl.semaphore_signal(known.at[2], inc=1, device_id=(up, sa), device_id_type=MESH)
            for device in x_line:
                pl.semaphore_signal(known.at[0], inc=1, device_id=device, device_id_type=MESH)
        chunk_sums(k, core, sown.at[k])

    def gate_d2d():
        return pltpu.make_async_remote_copy(
            src_ref=gall.at[4], dst_ref=gdrecv, send_sem=gd_sem.at[0], recv_sem=gd_sem.at[1],
            device_id=(partner, sa), device_id_type=MESH,
        )

    def gate_over():
        return pltpu.make_async_remote_copy(
            src_ref=gshard, dst_ref=gshard, send_sem=gd_sem.at[2], recv_sem=gd_sem.at[3],
            device_id=(partner, sa), device_id_type=MESH,
        )

    def gate_copy(which):
        return pltpu.make_async_remote_copy(
            src_ref=gall.at[zh], dst_ref=gall.at[zh],
            send_sem=gz_sem.at[0, which], recv_sem=gz_sem.at[1, which],
            device_id=((up, down, (row + 4) % 8)[which], sa), device_id_type=MESH,
        )

    gate_load.wait()
    gall[4] = gload[0] + gload[1]
    for r in range(2):
        rowsums[48 + 8 * r : 56 + 8 * r, :] = gload[r] * gload[r]

    prepare(0)
    prepare(1)

    @pl.when(core == 0)
    def _():
        pl.semaphore_wait(known.at[2], 1)

    d2d(0).wait_recv()
    scale = round_up(chip_top(0))
    factors = [put_scale(way, 0, scale) for way in range(2)]
    for piece in range(6):
        for way in range(2):
            zsend[way, 0, block(piece), :] = encoded(chip_rows(0, piece, way), factors[way])
            z_copy(way, 0, piece).start()


    @pl.when(core == 1)
    def _():
        pl.semaphore_wait(known.at[2], 1)
        gate_d2d().wait_recv()
        gall[zh] = gall[4] + gdrecv[...]
        for which in (2, 0, 1):
            gate_copy(which).start()


    prepare(2)
    pl.semaphore_wait(known.at[0], 3)
    pl.semaphore_signal(known.at[1], inc=1, device_id=z_pair, device_id_type=MESH)

    tops = []
    for way in range(2):
        k = 1 + way
        d2d(k).wait_recv()
        tops.append(chip_top(k))
        factor = put_scale(way, 1, round_up(tops[way]))
        for piece in range(6):
            zsend[way, 1, block(piece), :] = encoded(chip_rows(k, piece, 1 - way), factor)
        z_copy(way, 1, 0).start()

    prepare(3)

    factors = []
    for piece in range(6):
        for way in range(2):
            z_copy(way, 0, piece).wait_recv()
            if piece == 0:
                scale = round_up(tops[way] + z_scale(way, 0))
                factors.append(put_scale(way, 2, scale))
            values = chip_rows(1 + way, piece, way) + z_values(way, 0, piece)
            zsend[way, 2, block(piece), :] = encoded(values, factors[way])
            z_copy(way, 2, piece).start()

    @pl.when(core == 1)
    def _():
        for which in range(3):
            gate_copy(which).wait_recv()
        gate_total = ((gall[0] + gall[1]) + gall[2]) + gall[3]
        gshard[...] = (gate_total * (1 / 16)).astype(BF16)
        gate_over().start()

    @pl.when(core == 0)
    def _():
        gate_over().wait_recv()


    pl.semaphore_wait(known.at[1], 1)
    for peer in sa_peers:
        pltpu.make_async_remote_copy(
            src_ref=gshard, dst_ref=out_gate.at[:, pl.ds(pl.multiple_of(sa * 128, 128), 128)],
            send_sem=ga_sem.at[0], recv_sem=ga_sem.at[1],
            device_id=(row, peer), device_id_type=MESH,
        ).start()
    out_gate[:, pl.ds(pl.multiple_of(sa * 128, 128), 128)] = gshard[...]

    for t in range(3):
        part = squares[pl.ds(t * 128, 16, stride=8), :]
        for j in range(1, 8):
            part = part + squares[pl.ds(t * 128 + j, 16, stride=8), :]
        rowsums[16 * t : 16 * t + 16, :] = part
    rowsums[64:128, :] = jnp.zeros((64, 128), F32)
    norm_row = jnp.sum(rowsums[...].T, axis=0, keepdims=True)
    lane = lax.broadcasted_iota(jnp.int32, (1, 128), 1)

    def send_all(piece):
        for peer in sa_peers:
            pltpu.make_async_remote_copy(
                src_ref=msgs.at[piece, peer], dst_ref=recv.at[piece, sa],
                send_sem=ms_sem.at[piece], recv_sem=mr_sem.at[piece],
                device_id=(row, peer), device_id_type=MESH,
            ).start()
        recv[piece, sa] = msgs[piece, sa]

    d2d(3).wait_recv()
    for way in range(2):
        z_copy(way, 1, 0).wait_recv()
    for t in range(3):
        for part in range(2):
            for half in range(2):
                piece = 2 * t + part
                total = chip_rows(3, piece, half) + z_values(1 - half, 1, piece)
                z_copy(half, 2, piece).wait_recv()
                total = total + z_values(half, 2, piece)
                start = 64 * half + BLOCK * part
                served[t, start : start + BLOCK, :] = (total * (1 / 16)).astype(BF16).astype(F32)
        final = served[t]
        square = jnp.sum(final * final, axis=(0, 1), keepdims=True)
        norm_row = jnp.where(lane == 64 + t, square, norm_row)
        if t == 1:
            for p in range(32):
                parts = [served[j, 4 * p : 4 * p + 4, :] for j in range(2)]
                msgs[0, p] = jnp.concatenate(parts, axis=0).astype(BF16)
            send_all(0)

    high = norm_row.astype(BF16).astype(F32)
    rest = norm_row - high
    middle = rest.astype(BF16).astype(F32)
    tail = jnp.concatenate([high, middle, rest - middle, jnp.zeros((1, 128), F32)], axis=0)
    for p in range(32):
        msgs[1, p] = jnp.concatenate([served[2, 4 * p : 4 * p + 4, :], tail], axis=0).astype(BF16)
    send_all(1)

    for k in range(4):
        d2d(k).wait_send()
    for way in range(2):
        z_copy(way, 1, 0).wait_send()
        for stage in (0, 2):
            for piece in range(6):
                z_copy(way, stage, piece).wait_send()
    @pl.when(core == 0)
    def _():
        gate_d2d().wait_send()

    @pl.when(core == 1)
    def _():
        gate_over().wait_send()
        for which in range(3):
            gate_copy(which).wait_send()

    others = out_gate.at[:, pl.ds(0, 31 * 128)]
    pltpu.make_async_copy(others, others, ga_sem.at[0]).wait()
    pltpu.make_async_copy(others, others, ga_sem.at[1]).wait()

    for piece in range(2):
        batch = recv.at[piece, pl.ds(0, 31)]
        pltpu.make_async_copy(batch, batch, ms_sem.at[piece]).wait()
        pltpu.make_async_copy(batch, batch, mr_sem.at[piece]).wait()


def unpack(recv, gates, out_w1, out_w3, out_w2, out_gate, out_soup, out_rep):
    row = lax.axis_index("row")
    routed = gates[...]
    out_gate[...] = routed
    wide = routed.astype(F32)
    mine = lax.broadcasted_iota(jnp.int32, wide.shape, 0) == row
    gate_square = jnp.sum(jnp.where(mine, wide * wide, 0.0), axis=(0, 1), keepdims=True)

    totals = jnp.zeros((4, 128), F32)
    for s in range(32):
        columns = slice(128 * s, 128 * s + 128)
        first = recv[0, s].astype(F32)
        last = recv[1, s].astype(F32)
        out_w1[0, :, columns] = first[0:4].astype(BF16)
        out_w3[0, :, columns] = first[4:8].astype(BF16)
        out_w2[0, :, columns] = last[0:4].astype(BF16)
        totals = totals + last[4:8]
    total_row = (totals[0:1] + totals[1:2]) + totals[2:3]

    lane = lax.broadcasted_iota(jnp.int32, (1, 128), 1)
    for r in range(2):
        for t in range(4):
            entries = pltpu.roll(total_row, 128 - (16 * t + 8 * r) if t + r else 0, 1)
            norms = jnp.sqrt(entries * (1 / (4096 if t == 3 else 524288)))
            out_rep[r, t : t + 1, :] = norms[:, 0:8]
    soup = pltpu.roll(total_row, 64, 1) * (1 / 524288)
    soup = jnp.sqrt(jnp.where(lane == 3, gate_square * (1 / 4096), soup))
    out_soup[...] = soup[:, 0:4]


def body(w1, w3, w2, gate):
    vmem = pl.BlockSpec(memory_space=pltpu.VMEM)
    hbm = pl.BlockSpec(memory_space=pl.ANY)
    dma = pltpu.SemaphoreType.DMA
    recv, gates = pl.pallas_call(
        kernel,
        name="soup",
        out_shape=(
            pltpu.VMEM((2, 32, 8, 128), BF16),
            pltpu.VMEM((8, 4096), BF16),
        ),
        in_specs=[hbm] * 4,
        out_specs=(vmem,) * 2,
        scratch_shapes=[
            pltpu.VMEM((4, 3, 2, 2, 128, 128), F32),
            pltpu.VMEM((2, 8, 128), F32),
            pltpu.VMEM((4, 392, 128), F32),
            pltpu.VMEM((4, 392, 128), F32),
            pltpu.VMEM((4, 392, 128), F32),
            pltpu.VMEM((384, 128), F32),
            pltpu.VMEM((128, 128), F32),
            pltpu.VMEM((2, 3, FIRST + 192, 128), BF16),
            pltpu.VMEM((2, 3, FIRST + 192, 128), BF16),
            pltpu.VMEM((5, 8, 128), F32),
            pltpu.VMEM((8, 128), F32),
            pltpu.VMEM((8, 128), BF16),
            pltpu.VMEM((3, 128, 128), F32),
            pltpu.VMEM((2, 32, 8, 128), BF16),
            dma((4, 3)),
            dma,
            dma((4,)),
            dma((4,)),
            dma((2, 3, 6)),
            dma((2, 3, 6)),
            dma((4,)),
            dma((2, 3)),
            dma((2,)),
            dma((2,)),
            dma((2,)),
            pltpu.SemaphoreType.REGULAR((3,)),
        ],
        compiler_params=pltpu.CompilerParams(collective_id=0, has_side_effects=True, vmem_limit_bytes=56 * 2**20),
    )(w1, w3, w2, gate)
    outs = pl.pallas_call(
        unpack,
        name="unpack",
        out_shape=(
            jax.ShapeDtypeStruct((1, 4, 4096), BF16),
            jax.ShapeDtypeStruct((1, 4, 4096), BF16),
            jax.ShapeDtypeStruct((1, 4, 4096), BF16),
            jax.ShapeDtypeStruct((8, 4096), BF16),
            jax.ShapeDtypeStruct((1, 4), F32),
            jax.ShapeDtypeStruct((2, 4, 8), F32),
        ),
        in_specs=[vmem] * 2,
        out_specs=(vmem,) * 6,
        compiler_params=pltpu.CompilerParams(vmem_limit_bytes=4 * 2**20),
    )(recv, gates)
    return (*outs[:5], outs[5].transpose(0, 2, 1))


def solution(mesh):
    in_specs = (
        P("row", None, None, "sa"),
        P("row", None, None, "sa"),
        P("row", None, None, "sa"),
        P("row", None, "sa"),
    )
    out_specs = (
        P("row", "sa", None),
        P("row", "sa", None),
        P("row", "sa", None),
        P(),
        P("row", None),
        P("row", None, None),
    )
    return jax.shard_map(body, mesh=mesh, in_specs=in_specs, out_specs=out_specs, check_vma=False)
```

```python
import functools

import jax
import jax.numpy as jnp
from jax import lax
from jax.experimental import pallas as pl
from jax.experimental.pallas import tpu as pltpu
from jax.sharding import PartitionSpec as P

MESH = pl.DeviceIdType.MESH
F32, BF16 = jnp.float32, jnp.bfloat16

SPAN = 2.0**7.875


STEPS = sorted(
    [(dz, dx, dy) for dz in (0, 1) for dx in range(4) for dy in range(4) if dz + dx + dy],
    key=lambda d: -(d[0] + min(d[1], 4 - d[1]) + min(d[2], 4 - d[2])),
)
FIRST, BLOCK = 8, 32


def row_max(block8):
    return jnp.maximum(jnp.max(block8, axis=0, keepdims=True), 1e-30)


def round_up(scale):
    return (scale * 1.015625).astype(BF16)


def encoded(values, factor):
    u = values * factor
    u2 = u * u
    u4 = u2 * u2
    u8 = u4 * u4
    u16 = u8 * u8
    return jnp.where(u < 0, -u16, u16).astype(BF16)


def decoded(wire, factor):
    y = wire.astype(F32)
    root = lax.rsqrt(lax.rsqrt(lax.rsqrt(lax.rsqrt(jnp.abs(y)))))
    return jnp.where(y < 0, -root, root) * factor


def kernel(
    w1, w3, w2, gate,
    recv, out_gate,
    load, gload, sown, dsend, drecv, squares, rowsums,
    zsend, zrecv, gall, gdrecv, gshard, served, msgs,
    load_sem, gload_sem, ds_sem, dr_sem, zs_sem, zr_sem, gd_sem, gz_sem, ga_sem, ms_sem, mr_sem, known,
):
    weights = (w1, w3, w2)
    row, sa = lax.axis_index("row"), lax.axis_index("sa")
    zh, core = row // 2, row % 2
    partner = row + 1 - 2 * core
    up, down = (row + 2) % 8, (row + 6) % 8

    chips = [(zh + d) % 4 for d in (2, 1, 3, 0)]

    def load_copy(k, t):
        return pltpu.make_async_copy(
            weights[t].at[:, pl.ds(2 * chips[k], 2)], load.at[k, t], load_sem.at[k, t]
        )

    gate_load = pltpu.make_async_copy(gate, gload, gload_sem)
    gate_load.start()
    for t in range(3):
        load_copy(0, t).start()

    zl, x, y = sa // 16, (sa // 4) % 4, sa % 4
    zs, xs, ys = [zl * 16, 16 - zl * 16], [((x + i) % 4) * 4 for i in range(4)], [(y + i) % 4 for i in range(4)]
    x_line = [(row, zs[0] + xs[i] + y) for i in (1, 2, 3)]
    y_line = [(row, zs[0] + xs[0] + ys[i]) for i in (1, 2, 3)]
    z_pair = (row, zs[1] + xs[0] + y)
    sa_peers = [zs[dz] + xs[dx] + ys[dy] for dz, dx, dy in STEPS]
    barrier = pltpu.get_barrier_semaphore()
    for device in [(up, sa), (down, sa), (partner, sa), *x_line, *y_line, z_pair]:
        pl.semaphore_signal(barrier, inc=1, device_id=device, device_id_type=MESH)
    for k in range(1, 4):
        for t in range(3):
            load_copy(k, t).start()

    def chunk_sums(k, parity, dest):
        expert = 2 * chips[k] + parity
        top = jnp.zeros((8, 128), F32)
        for t in range(3):
            a, b = load[k, t, 0, parity], load[k, t, 1, parity]
            total = a + b
            dest[8 + t * 128 : 136 + t * 128, :] = total
            for r, v in ((0, a), (1, b)):
                index = pl.multiple_of((t * 16 + r * 8 + expert) * 8, 8)
                squares[pl.ds(index, 8), :] = jnp.sum((v * v).reshape(16, 8, 128), axis=0)
            if k < 3:
                top = jnp.maximum(top, jnp.max(jnp.abs(total).reshape(16, 8, 128), axis=0))
        if k < 3:
            dest[0:8, :] = top

    def d2d(k, rest=False):
        rows = pl.ds(0, 392) if k else pl.ds(136, 256) if rest else pl.ds(0, 136)
        slot = 4 if rest else k
        return pltpu.make_async_remote_copy(
            src_ref=dsend.at[k, rows], dst_ref=drecv.at[k, rows],
            send_sem=ds_sem.at[slot], recv_sem=dr_sem.at[slot],
            device_id=(partner, sa), device_id_type=MESH,
        )

    def z_copy(way, stage, piece):
        if stage == 1:
            rows = pl.ds(0, FIRST + 192)
        elif piece == 0:
            rows = pl.ds(0, FIRST + BLOCK)
        else:
            rows = pl.ds(FIRST + BLOCK * piece, BLOCK)
        return pltpu.make_async_remote_copy(
            src_ref=zsend.at[way, stage, rows], dst_ref=zrecv.at[way, stage, rows],
            send_sem=zs_sem.at[way, stage, piece], recv_sem=zr_sem.at[way, stage, piece],
            device_id=((up, down)[way], sa), device_id_type=MESH,
        )

    def chip_rows(k, piece, half):
        t, part = piece // 2, piece % 2
        start = 8 + t * 128 + half * 64 + part * BLOCK
        return sown[k, start : start + BLOCK, :] + drecv[k, start : start + BLOCK, :]

    def chip_top(k):
        return row_max(sown[k, 0:8, :] + drecv[k, 0:8, :])

    def put_scale(way, stage, scale):
        zsend[way, stage, 0:FIRST, :] = jnp.broadcast_to(scale, (FIRST, 128))
        return SPAN / scale.astype(F32)

    def block(piece):
        return slice(FIRST + BLOCK * piece, FIRST + BLOCK * piece + BLOCK)

    def z_scale(way, stage):
        return zrecv[way, stage, 0:FIRST, :].astype(F32)[0:1]

    def z_values(way, stage, piece):
        return decoded(zrecv[way, stage, block(piece), :], z_scale(way, stage) * (1 / SPAN))

    def prepare(k):
        for t in range(3):
            load_copy(k, t).wait()
        chunk_sums(k, 1 - core, dsend.at[k])
        if k == 0:
            pl.semaphore_wait(barrier, 10)
        d2d(k).start()
        if k == 0:
            d2d(0, True).start()
        if k == 0:

            @pl.when(core == 0)
            def _():
                gate_d2d().start()

            pl.semaphore_signal(known.at[2], inc=1, device_id=(up, sa), device_id_type=MESH)
            for device in x_line:
                pl.semaphore_signal(known.at[0], inc=1, device_id=device, device_id_type=MESH)
        chunk_sums(k, core, sown.at[k])

    def gate_d2d():
        return pltpu.make_async_remote_copy(
            src_ref=gall.at[4], dst_ref=gdrecv, send_sem=gd_sem.at[0], recv_sem=gd_sem.at[1],
            device_id=(partner, sa), device_id_type=MESH,
        )

    def gate_over():
        return pltpu.make_async_remote_copy(
            src_ref=gshard, dst_ref=gshard, send_sem=gd_sem.at[2], recv_sem=gd_sem.at[3],
            device_id=(partner, sa), device_id_type=MESH,
        )

    def gate_copy(which):
        return pltpu.make_async_remote_copy(
            src_ref=gall.at[zh], dst_ref=gall.at[zh],
            send_sem=gz_sem.at[0, which], recv_sem=gz_sem.at[1, which],
            device_id=((up, down, (row + 4) % 8)[which], sa), device_id_type=MESH,
        )

    gate_load.wait()
    gall[4] = gload[0] + gload[1]
    for r in range(2):
        rowsums[48 + 8 * r : 56 + 8 * r, :] = gload[r] * gload[r]

    prepare(0)
    prepare(1)

    @pl.when(core == 0)
    def _():
        pl.semaphore_wait(known.at[2], 1)

    d2d(0).wait_recv()
    scale = round_up(chip_top(0))
    factors = [put_scale(way, 0, scale) for way in range(2)]
    for piece in range(6):
        if piece == 2:
            d2d(0, True).wait_recv()
        for way in range(2):
            zsend[way, 0, block(piece), :] = encoded(chip_rows(0, piece, way), factors[way])
            z_copy(way, 0, piece).start()


    @pl.when(core == 1)
    def _():
        pl.semaphore_wait(known.at[2], 1)
        gate_d2d().wait_recv()
        gall[zh] = gall[4] + gdrecv[...]
        for which in (2, 0, 1):
            gate_copy(which).start()


    prepare(2)
    pl.semaphore_wait(known.at[0], 3)
    pl.semaphore_signal(known.at[1], inc=1, device_id=z_pair, device_id_type=MESH)

    tops = []
    for way in range(2):
        k = 1 + way
        d2d(k).wait_recv()
        tops.append(chip_top(k))
        factor = put_scale(way, 1, round_up(tops[way]))
        for piece in range(6):
            zsend[way, 1, block(piece), :] = encoded(chip_rows(k, piece, 1 - way), factor)
        z_copy(way, 1, 0).start()

    prepare(3)

    factors = []
    for piece in range(6):
        for way in range(2):
            z_copy(way, 0, piece).wait_recv()
            if piece == 0:
                scale = round_up(tops[way] + z_scale(way, 0))
                factors.append(put_scale(way, 2, scale))
            values = chip_rows(1 + way, piece, way) + z_values(way, 0, piece)
            zsend[way, 2, block(piece), :] = encoded(values, factors[way])
            z_copy(way, 2, piece).start()

    @pl.when(core == 1)
    def _():
        for which in range(3):
            gate_copy(which).wait_recv()
        gate_total = ((gall[0] + gall[1]) + gall[2]) + gall[3]
        gshard[...] = (gate_total * (1 / 16)).astype(BF16)
        gate_over().start()

    @pl.when(core == 0)
    def _():
        gate_over().wait_recv()


    pl.semaphore_wait(known.at[1], 1)
    for peer in sa_peers:
        pltpu.make_async_remote_copy(
            src_ref=gshard, dst_ref=out_gate.at[:, pl.ds(pl.multiple_of(sa * 128, 128), 128)],
            send_sem=ga_sem.at[0], recv_sem=ga_sem.at[1],
            device_id=(row, peer), device_id_type=MESH,
        ).start()
    out_gate[:, pl.ds(pl.multiple_of(sa * 128, 128), 128)] = gshard[...]

    for t in range(3):
        part = squares[pl.ds(t * 128, 16, stride=8), :]
        for j in range(1, 8):
            part = part + squares[pl.ds(t * 128 + j, 16, stride=8), :]
        rowsums[16 * t : 16 * t + 16, :] = part
    rowsums[64:128, :] = jnp.zeros((64, 128), F32)
    norm_row = jnp.sum(rowsums[...].T, axis=0, keepdims=True)
    lane = lax.broadcasted_iota(jnp.int32, (1, 128), 1)

    def send_all(piece):
        for peer in sa_peers:
            pltpu.make_async_remote_copy(
                src_ref=msgs.at[piece, peer], dst_ref=recv.at[piece, sa],
                send_sem=ms_sem.at[piece], recv_sem=mr_sem.at[piece],
                device_id=(row, peer), device_id_type=MESH,
            ).start()
        recv[piece, sa] = msgs[piece, sa]

    d2d(3).wait_recv()
    for way in range(2):
        z_copy(way, 1, 0).wait_recv()
    for t in range(3):
        for part in range(2):
            for half in range(2):
                piece = 2 * t + part
                total = chip_rows(3, piece, half) + z_values(1 - half, 1, piece)
                z_copy(half, 2, piece).wait_recv()
                total = total + z_values(half, 2, piece)
                start = 64 * half + BLOCK * part
                served[t, start : start + BLOCK, :] = (total * (1 / 16)).astype(BF16).astype(F32)
        final = served[t]
        square = jnp.sum(final * final, axis=(0, 1), keepdims=True)
        norm_row = jnp.where(lane == 64 + t, square, norm_row)
        if t == 1:
            for p in range(32):
                parts = [served[j, 4 * p : 4 * p + 4, :] for j in range(2)]
                msgs[0, p] = jnp.concatenate(parts, axis=0).astype(BF16)
            send_all(0)

    high = norm_row.astype(BF16).astype(F32)
    rest = norm_row - high
    middle = rest.astype(BF16).astype(F32)
    tail = jnp.concatenate([high, middle, rest - middle, jnp.zeros((1, 128), F32)], axis=0)
    for p in range(32):
        msgs[1, p] = jnp.concatenate([served[2, 4 * p : 4 * p + 4, :], tail], axis=0).astype(BF16)
    send_all(1)

    for k in range(4):
        d2d(k).wait_send()
    d2d(0, True).wait_send()
    for way in range(2):
        z_copy(way, 1, 0).wait_send()
        for stage in (0, 2):
            for piece in range(6):
                z_copy(way, stage, piece).wait_send()
    @pl.when(core == 0)
    def _():
        gate_d2d().wait_send()

    @pl.when(core == 1)
    def _():
        gate_over().wait_send()
        for which in range(3):
            gate_copy(which).wait_send()

    others = out_gate.at[:, pl.ds(0, 31 * 128)]
    pltpu.make_async_copy(others, others, ga_sem.at[0]).wait()
    pltpu.make_async_copy(others, others, ga_sem.at[1]).wait()

    for piece in range(2):
        batch = recv.at[piece, pl.ds(0, 31)]
        pltpu.make_async_copy(batch, batch, ms_sem.at[piece]).wait()
        pltpu.make_async_copy(batch, batch, mr_sem.at[piece]).wait()


def unpack(recv, gates, out_w1, out_w3, out_w2, out_gate, out_soup, out_rep):
    row = lax.axis_index("row")
    routed = gates[...]
    out_gate[...] = routed
    wide = routed.astype(F32)
    mine = lax.broadcasted_iota(jnp.int32, wide.shape, 0) == row
    gate_square = jnp.sum(jnp.where(mine, wide * wide, 0.0), axis=(0, 1), keepdims=True)

    totals = jnp.zeros((4, 128), F32)
    for s in range(32):
        columns = slice(128 * s, 128 * s + 128)
        first = recv[0, s].astype(F32)
        last = recv[1, s].astype(F32)
        out_w1[0, :, columns] = first[0:4].astype(BF16)
        out_w3[0, :, columns] = first[4:8].astype(BF16)
        out_w2[0, :, columns] = last[0:4].astype(BF16)
        totals = totals + last[4:8]
    total_row = (totals[0:1] + totals[1:2]) + totals[2:3]

    lane = lax.broadcasted_iota(jnp.int32, (1, 128), 1)
    for r in range(2):
        for t in range(4):
            entries = pltpu.roll(total_row, 128 - (16 * t + 8 * r) if t + r else 0, 1)
            norms = jnp.sqrt(entries * (1 / (4096 if t == 3 else 524288)))
            out_rep[r, t : t + 1, :] = norms[:, 0:8]
    soup = pltpu.roll(total_row, 64, 1) * (1 / 524288)
    soup = jnp.sqrt(jnp.where(lane == 3, gate_square * (1 / 4096), soup))
    out_soup[...] = soup[:, 0:4]


def body(w1, w3, w2, gate):
    vmem = pl.BlockSpec(memory_space=pltpu.VMEM)
    hbm = pl.BlockSpec(memory_space=pl.ANY)
    dma = pltpu.SemaphoreType.DMA
    recv, gates = pl.pallas_call(
        kernel,
        name="soup",
        out_shape=(
            pltpu.VMEM((2, 32, 8, 128), BF16),
            pltpu.VMEM((8, 4096), BF16),
        ),
        in_specs=[hbm] * 4,
        out_specs=(vmem,) * 2,
        scratch_shapes=[
            pltpu.VMEM((4, 3, 2, 2, 128, 128), F32),
            pltpu.VMEM((2, 8, 128), F32),
            pltpu.VMEM((4, 392, 128), F32),
            pltpu.VMEM((4, 392, 128), F32),
            pltpu.VMEM((4, 392, 128), F32),
            pltpu.VMEM((384, 128), F32),
            pltpu.VMEM((128, 128), F32),
            pltpu.VMEM((2, 3, FIRST + 192, 128), BF16),
            pltpu.VMEM((2, 3, FIRST + 192, 128), BF16),
            pltpu.VMEM((5, 8, 128), F32),
            pltpu.VMEM((8, 128), F32),
            pltpu.VMEM((8, 128), BF16),
            pltpu.VMEM((3, 128, 128), F32),
            pltpu.VMEM((2, 32, 8, 128), BF16),
            dma((4, 3)),
            dma,
            dma((5,)),
            dma((5,)),
            dma((2, 3, 6)),
            dma((2, 3, 6)),
            dma((4,)),
            dma((2, 3)),
            dma((2,)),
            dma((2,)),
            dma((2,)),
            pltpu.SemaphoreType.REGULAR((3,)),
        ],
        compiler_params=pltpu.CompilerParams(collective_id=0, has_side_effects=True, vmem_limit_bytes=56 * 2**20),
    )(w1, w3, w2, gate)
    outs = pl.pallas_call(
        unpack,
        name="unpack",
        out_shape=(
            jax.ShapeDtypeStruct((1, 4, 4096), BF16),
            jax.ShapeDtypeStruct((1, 4, 4096), BF16),
            jax.ShapeDtypeStruct((1, 4, 4096), BF16),
            jax.ShapeDtypeStruct((8, 4096), BF16),
            jax.ShapeDtypeStruct((1, 4), F32),
            jax.ShapeDtypeStruct((2, 4, 8), F32),
        ),
        in_specs=[vmem] * 2,
        out_specs=(vmem,) * 6,
        compiler_params=pltpu.CompilerParams(vmem_limit_bytes=4 * 2**20),
    )(recv, gates)
    return (*outs[:5], outs[5].transpose(0, 2, 1))


def solution(mesh):
    in_specs = (
        P("row", None, None, "sa"),
        P("row", None, None, "sa"),
        P("row", None, None, "sa"),
        P("row", None, "sa"),
    )
    out_specs = (
        P("row", "sa", None),
        P("row", "sa", None),
        P("row", "sa", None),
        P(),
        P("row", None),
        P("row", None, None),
    )
    return jax.shard_map(body, mesh=mesh, in_specs=in_specs, out_specs=out_specs, check_vma=False)
```
